16 devices in a mesh: col: 2 (over z), row: 8 (over y, x, core).
Axes of the slice: x: 2, y: 2, z: 2, core: 2. Of those that a mesh axis runs over, the one named last changes fastest.
Arguments:
- trans_mat: bfloat16 [24576, 24576], P('row', 'col')
- x_start: float32 [24576, 256], P(('col', 'row'))
- teleport: float32 [24576, 256], P(('col', 'row'))
- dangling: int32 [24576], P(('col', 'row'))
Outputs:
- output: float32 [24576, 256], P(('col', 'row'))
All inputs are finite; a program needn't handle non-finite values.
Results may differ from the reference program's by a relative error of at most 0.001.
Values are sent between devices in bfloat16 or wider.
A program may use at most 1 GiB of HBM per device.

```python
import jax
import jax.numpy as jnp
from jax import lax

VERTICES = 24576
VECS = 256
DEGREE = 7
SWEEPS = 8
DAMPING = 0.85


def draw_graph(key_dang, key_target, key_edge):
    dangling = (jax.random.randint(key_dang, (VERTICES,), 0, 5) == 0).astype(jnp.int32)
    live_cols = (1 - dangling).astype(jnp.bfloat16)
    target = jax.random.randint(key_target, (VERTICES,), 0, VERTICES)
    row_blocks = 16
    block_rows = VERTICES // row_blocks
    block_keys = jax.random.split(key_edge, row_blocks)
    block_starts = jnp.arange(row_blocks, dtype=jnp.int32) * block_rows

    def edge_block(block_args):
        block_key, block_start = block_args
        draw_vals = jax.random.randint(block_key, (block_rows, VERTICES), 0, VERTICES)
        row_ids = block_start + jnp.arange(block_rows, dtype=jnp.int32)[:, None]
        edge_mask = (draw_vals < DEGREE) | (row_ids == target[None, :])
        return edge_mask.astype(jnp.bfloat16) * live_cols[None, :]

    adjacency = lax.map(edge_block, (block_keys, block_starts)).reshape(VERTICES, VERTICES)
    out_degree = jnp.sum(adjacency, axis=0, dtype=jnp.float32)
    inv_degree = (1.0 / jnp.maximum(out_degree, 1.0)).astype(jnp.bfloat16)
    trans_mat = adjacency * inv_degree[None, :]
    return trans_mat, dangling


def setup_inputs(seed: int = 0) -> dict:
    base_key = jax.random.key(seed)
    k_dang, k_target, k_edge, k_start, k_scale, k_center, k_weight = jax.random.split(base_key, 7)
    trans_mat, dangling = draw_graph(k_dang, k_target, k_edge)
    col_scale = 2.0 ** jax.random.uniform(k_scale, (1, VECS), jnp.float32, -2.0, 2.0)
    x_start = jax.random.uniform(k_start, (VERTICES, VECS), jnp.float32, 0.0, 2.0) * col_scale
    centers = jax.random.randint(k_center, (1, VECS), 0, VERTICES)
    offsets = (jnp.arange(VERTICES, dtype=jnp.int32)[:, None] - centers) % VERTICES
    inside = (offsets < VERTICES // 8).astype(jnp.float32)
    raw_tele = inside * jax.random.uniform(k_weight, (VERTICES, VECS), jnp.float32, 0.5, 2.0)
    teleport = raw_tele * (VERTICES / jnp.sum(raw_tele, axis=0, keepdims=True))
    return {'trans_mat': trans_mat, 'x_start': x_start, 'teleport': teleport, 'dangling': dangling}


def reference(trans_mat, x_start, teleport, dangling):
    dang_col = dangling.astype(jnp.float32)[:, None]

    def one_sweep(x_cur, unused):
        dang_mass = jnp.sum(dang_col * x_cur, axis=0) / VERTICES
        spread = jnp.dot(trans_mat, x_cur.astype(jnp.bfloat16), preferred_element_type=jnp.float32)
        x_next = DAMPING * spread + (DAMPING * dang_mass + (1.0 - DAMPING))[None, :] * teleport
        return x_next, None

    x_final, unused_out = lax.scan(one_sweep, x_start, None, length=SWEEPS)
    return x_final
```

```python
import functools

import jax
import jax.numpy as jnp
from jax import lax
from jax.experimental import pallas as pl
from jax.experimental.pallas import tpu as pltpu
from jax.sharding import PartitionSpec as P

SWEEPS = 8
DAMPING = 0.85
CH = 128
LAG = 4
SLOTS = 3
MT = 512
MB = 256
MESH = pl.DeviceIdType.MESH


def sweeps_kernel(steps, a_ref, x0_ref, v_ref, dang_ref, s0_ref, o_ref,
                  abuf, xbuf, xst, yacc, zr, spart, sbuf, svec,
                  a_sem, x0_sem, z_send, z_recv, r_send, r_recv, y_send, y_recv, x_send, x_recv,
                  d1_send, d1_recv, d2_send, d2_recv, s_send, s_recv):
    i = lax.axis_index('row')
    z = lax.axis_index('col')
    y, x, c = i // 4, (i // 2) % 2, i % 2
    me = z * 8 + i
    home = z == y
    away = z != y
    part = jnp.where(home, 0, 1)
    k_own = 2 * x + c
    k_sib = 2 * x + 1 - c
    k_x = 2 * (1 - x) + c
    k_d = 2 * (1 - x) + 1 - c
    z_dev = {'col': 1 - z, 'row': i}
    sib_dev = {'col': z, 'row': i + 1 - 2 * c}
    x_dev = {'col': z, 'row': i + 2 - 4 * x}
    y_dev = {'col': z, 'row': i + 4 - 8 * y}
    piece = steps * CH
    vertices = 16 * piece

    def other(off):
        dev = (me + off) % 16
        return {'col': dev // 8, 'row': dev % 8}, dev

    barrier = pltpu.get_barrier_semaphore()

    @pl.loop(1, 16)
    def _(off):
        dev, _ = other(off)
        pl.semaphore_signal(barrier, inc=1, device_id=dev, device_id_type=MESH)

    pl.semaphore_wait(barrier, 15)

    def remote(src, dst, send, recv, dev):
        return pltpu.make_async_remote_copy(src_ref=src, dst_ref=dst, send_sem=send, recv_sem=recv,
                                            device_id=dev, device_id_type=MESH)

    def z_copy(t, q):
        rows = pl.ds(pl.multiple_of((1 - part) * piece + q * CH, CH), CH)
        return remote(yacc.at[t, rows], zr.at[t, pl.ds(pl.multiple_of(q * CH, CH), CH)],
                      z_send.at[t, q], z_recv.at[t, q], z_dev)

    def r_copy(p, q):
        return remote(xst.at[p, q], xbuf.at[p, q, k_own, 1], r_send.at[p, q], r_recv.at[p, q], z_dev)

    def y_copy(p, q):
        return remote(xbuf.at[p, q, k_own], xbuf.at[p, q, k_own], y_send.at[p, q], y_recv.at[p, q], y_dev)

    def x_copy(p, q):
        return remote(xbuf.at[p, q, k_own], xbuf.at[p, q, k_own], x_send.at[p, q], x_recv.at[p, q], x_dev)

    def d1_copy(p, q):
        return remote(xbuf.at[p, q, k_own], xbuf.at[p, q, k_own], d1_send.at[p, q], d1_recv.at[p, q], sib_dev)

    def d2_copy(p, q):
        return remote(xbuf.at[p, q, k_x], xbuf.at[p, q, k_x], d2_send.at[p, q], d2_recv.at[p, q], sib_dev)

    def landed(ref, sem):
        pltpu.make_async_copy(ref, ref, sem).wait()

    def a_start(g):
        q = lax.rem(g, steps)
        slot = lax.rem(g, SLOTS)
        for b in range(8):
            cols = pl.ds(pl.multiple_of(b * piece + q * CH, CH), CH)
            pltpu.make_async_copy(a_ref.at[:, cols], abuf.at[slot, :, pl.ds(b * CH, CH)], a_sem.at[slot]).start()

    def a_next(g):
        @pl.when(g + SLOTS < SWEEPS * steps)
        def _():
            a_start(g + SLOTS)

    def block_x(p, q):
        return xbuf[p, q].reshape(8 * CH, xbuf.shape[-1])

    def multiply(p, q, g):
        slot = lax.rem(g, SLOTS)
        landed(abuf.at[slot], a_sem.at[slot])

        @pl.loop(0, 2 * piece // MT)
        def _(m):
            rows = pl.ds(pl.multiple_of(m * MT, MT), MT)
            yacc[p, rows] += jnp.dot(abuf[slot, rows], block_x(p, q), preferred_element_type=jnp.float32)

        a_next(g)

    def multiply_last(p, g):
        slot = lax.rem(g, SLOTS)
        landed(abuf.at[slot], a_sem.at[slot])
        x_last = block_x(p, steps - 1)

        @pl.loop(0, piece // MB)
        def _(m):
            for which in (1 - part, part):
                rows = pl.ds(pl.multiple_of(which * piece + m * MB, MB), MB)
                yacc[p, rows] += jnp.dot(abuf[slot, rows], x_last, preferred_element_type=jnp.float32)

            @pl.when(m == 0)
            def _():
                z_copy(p, 0).start()
                z_copy(p, 1).start()

        a_next(g)

    def clear(p):
        @pl.loop(0, 2 * piece // MB)
        def _(m):
            rows = pl.ds(pl.multiple_of(m * MB, MB), MB)
            yacc[p, rows] = jnp.zeros((MB, yacc.shape[-1]), jnp.float32)

    def new_rows(t, q):
        rows = pl.ds(pl.multiple_of(q * CH, CH), CH)
        mine = pl.ds(pl.multiple_of(part * piece + q * CH, CH), CH)
        landed(zr.at[t, rows], z_recv.at[t, q])
        return DAMPING * (yacc[t, mine] + zr[t, rows]) + svec[0:1] * v_ref[rows], rows

    @pl.loop(0, SLOTS)
    def _(g):
        a_start(g)

    @pl.loop(0, steps)
    def _(q):
        pltpu.make_async_copy(x0_ref.at[:, :, q], xbuf.at[0, q], x0_sem.at[q]).start()

    svec[...] = jnp.broadcast_to(DAMPING * s0_ref[...] + (1.0 - DAMPING), svec.shape)
    clear(0)

    @pl.loop(0, steps - 1)
    def _(q):
        landed(xbuf.at[0, q], x0_sem.at[q])
        multiply(0, q, q)

    landed(xbuf.at[0, steps - 1], x0_sem.at[steps - 1])
    multiply_last(0, steps - 1)

    @pl.loop(0, SWEEPS - 1)
    def _(sweep):
        t = lax.rem(sweep, 2)
        p = 1 - t

        @pl.when(sweep > 0)
        def _():
            @pl.loop(1, 16)
            def _(off):
                _, dev = other(off)
                landed(sbuf.at[t, dev], s_recv.at[t, dev])

            s_sum = jnp.sum(sbuf[t].reshape(16 * 8, sbuf.shape[-1]), axis=0, keepdims=True) / vertices
            svec[...] = jnp.broadcast_to(DAMPING * s_sum + (1.0 - DAMPING), svec.shape)

        clear(p)
        spart[p] = jnp.zeros(spart.shape[1:], jnp.float32)

        @pl.loop(0, steps + LAG)
        def _(step):
            @pl.when(step + 2 < steps)
            def _():
                z_copy(t, step + 2).start()

            @pl.when(step < steps)
            def _():
                q = step
                rows_new, rows = new_rows(t, q)
                rows_bf = rows_new.astype(jnp.bfloat16)

                @pl.when(home)
                def _():
                    xbuf[p, q, k_own, 0] = rows_bf

                @pl.when(away)
                def _():
                    xst[p, q] = rows_bf

                spart[p] += jnp.sum((dang_ref[rows] * rows_new).reshape(CH // 8, 8, rows_new.shape[-1]), axis=0)

                @pl.when(away)
                def _():
                    r_copy(p, q).start()

            @pl.when(step == steps - 1)
            def _():
                sbuf[p, me] = spart[p]

                @pl.loop(1, 16)
                def _(off):
                    dev, _ = other(off)
                    remote(spart.at[p], sbuf.at[p, me], s_send.at[p, off], s_recv.at[p, me], dev).start()

            @pl.when((step >= 1) & (step < steps + 1) & home)
            def _():
                q = step - 1
                landed(xst.at[p, q], r_recv.at[p, q])
                y_copy(p, q).start()
                x_copy(p, q).start()
                d1_copy(p, q).start()

            @pl.when((step >= 2) & (step < steps + 2) & away)
            def _():
                q = step - 2
                landed(xbuf.at[p, q, k_own], y_recv.at[p, q])
                x_copy(p, q).start()
                d1_copy(p, q).start()

            @pl.when((step >= 3) & (step < steps + 3))
            def _():
                q = step - 3
                landed(xbuf.at[p, q, k_x], x_recv.at[p, q])
                d2_copy(p, q).start()

            @pl.when(step >= 4)
            def _():
                q = step - 4
                landed(xbuf.at[p, q, k_sib], d1_recv.at[p, q])
                landed(xbuf.at[p, q, k_d], d2_recv.at[p, q])

                @pl.when(q < steps - 1)
                def _():
                    multiply(p, q, (sweep + 1) * steps + q)

        multiply_last(p, (sweep + 1) * steps + steps - 1)

        @pl.loop(0, steps)
        def _(q):
            z_copy(t, q).wait_send()
            x_copy(p, q).wait_send()
            d1_copy(p, q).wait_send()
            d2_copy(p, q).wait_send()

            @pl.when(home)
            def _():
                y_copy(p, q).wait_send()

            @pl.when(away)
            def _():
                r_copy(p, q).wait_send()

        @pl.loop(1, 16)
        def _(off):
            dev, _ = other(off)
            remote(spart.at[p], sbuf.at[p, me], s_send.at[p, off], s_recv.at[p, me], dev).wait_send()

    t = (SWEEPS - 1) % 2

    @pl.loop(1, 16)
    def _(off):
        _, dev = other(off)
        landed(sbuf.at[t, dev], s_recv.at[t, dev])

    s_sum = jnp.sum(sbuf[t].reshape(16 * 8, sbuf.shape[-1]), axis=0, keepdims=True) / vertices
    svec[...] = jnp.broadcast_to(DAMPING * s_sum + (1.0 - DAMPING), svec.shape)

    @pl.loop(0, steps)
    def _(q):
        @pl.when(q + 2 < steps)
        def _():
            z_copy(t, q + 2).start()

        rows_new, rows = new_rows(t, q)
        o_ref[rows] = rows_new

    @pl.loop(0, steps)
    def _(q):
        z_copy(t, q).wait_send()


def solution(mesh):
    def piece_of(dev):
        z, i = dev // 8, dev % 8
        return 2 * i + (0 if z == i // 4 else 1)

    to_sums = [(piece_of(dev), dev) for dev in range(16)]
    from_sums = [(dev, piece_of(dev)) for dev in range(16)]

    def local_sweeps(mat_tile, x_piece, tele_piece, dang_piece):
        piece, vecs = x_piece.shape
        steps = piece // CH
        vertex_count = 16 * piece
        dang_col = dang_piece.astype(jnp.float32)[:, None]
        s0 = lax.psum(jnp.sum(dang_col * x_piece, axis=0, keepdims=True), ('col', 'row')) / vertex_count
        x_src = lax.all_gather(x_piece.astype(jnp.bfloat16), 'row', axis=0, tiled=True)
        x_src = x_src.reshape(4, 2, steps, CH, vecs)
        tele = lax.ppermute(tele_piece, ('col', 'row'), perm=to_sums)
        dang = lax.ppermute(dang_piece, ('col', 'row'), perm=to_sums).astype(jnp.float32)[:, None]
        sems = pltpu.SemaphoreType.DMA
        out = pl.pallas_call(
            functools.partial(sweeps_kernel, steps),
            out_shape=jax.ShapeDtypeStruct((piece, vecs), jnp.float32),
            in_specs=[pl.BlockSpec(memory_space=pl.ANY), pl.BlockSpec(memory_space=pl.ANY)]
            + [pl.BlockSpec(memory_space=pltpu.VMEM)] * 3,
            out_specs=pl.BlockSpec(memory_space=pltpu.VMEM),
            scratch_shapes=[
                pltpu.VMEM((SLOTS, 2 * piece, 8 * CH), jnp.bfloat16),
                pltpu.VMEM((2, steps, 4, 2, CH, vecs), jnp.bfloat16),
                pltpu.VMEM((2, steps, CH, vecs), jnp.bfloat16),
                pltpu.VMEM((2, 2 * piece, vecs), jnp.float32),
                pltpu.VMEM((2, piece, vecs), jnp.float32),
                pltpu.VMEM((2, 8, vecs), jnp.float32),
                pltpu.VMEM((2, 16, 8, vecs), jnp.float32),
                pltpu.VMEM((8, vecs), jnp.float32),
                sems((SLOTS,)), sems((steps,)),
            ] + [sems((2, steps))] * 12 + [sems((2, 16))] * 2,
            compiler_params=pltpu.CompilerParams(collective_id=0, has_side_effects=True,
                                                 vmem_limit_bytes=67_000_000),
            name='sweeps',
        )(mat_tile, x_src, tele, dang, s0)
        return lax.ppermute(out, ('col', 'row'), perm=from_sums)

    vec_spec = P(('col', 'row'), None)
    return jax.shard_map(local_sweeps, mesh=mesh,
                         in_specs=(P('row', 'col'), vec_spec, vec_spec, P(('col', 'row'))),
                         out_specs=vec_spec, check_vma=False)
```

```python
import jax
import jax.numpy as jnp
from jax import lax
from jax.experimental import pallas as pl
from jax.experimental.pallas import tpu as pltpu
from jax.sharding import PartitionSpec as P

SWEEPS = 8
DAMPING = 0.85
CH = 64
BR = 128
LAG = 2
AHEAD = 3
SLOTS = 3
MT = 512
MB = 256
VAHEAD = 3
MESH = pl.DeviceIdType.MESH


def sweeps_kernel(a_ref, x_ref, v_ref, dang_ref, o_ref,
                  abuf, xbuf, xst, yacc, zr, vperm, dperm, dcol, spart, sbuf, svec,
                  a_sem, g_send, gx_recv, gy_recv, gd_recv, gs_recv, v_send, v_recv, dang_sem, o_send, o_recv,
                  z_send, z_recv, r_send, r_recv, y_send, y_recv, x_send, x_recv,
                  d1_send, d1_recv, d2_send, d2_recv, s_send, s_recv):
    i = lax.axis_index('row')
    z = lax.axis_index('col')
    y, x, c = i // 4, (i // 2) % 2, i % 2
    me = z * 8 + i
    home = z == y
    away = z != y
    part = jnp.where(home, 0, 1)
    k_own = 2 * x + c
    k_sib = 2 * x + 1 - c
    k_x = 2 * (1 - x) + c
    k_d = 2 * (1 - x) + 1 - c
    sib_dev = {'col': z, 'row': i + 1 - 2 * c}
    x_dev = {'col': z, 'row': i + 2 - 4 * x}
    y_row = i + 4 - 8 * y
    y_dev = {'col': z, 'row': y_row}
    z_dev = {'col': 1 - z, 'row': i}
    piece, vecs = o_ref.shape
    chunks = piece // CH
    blocks = piece // BR
    per = BR // CH
    vertices = 16 * piece

    def other(off):
        dev = (me + off) % 16
        return {'col': dev // 8, 'row': dev % 8}, dev

    barrier = pltpu.get_barrier_semaphore()

    @pl.loop(1, 16)
    def _(off):
        dev, _ = other(off)
        pl.semaphore_signal(barrier, inc=1, device_id=dev, device_id_type=MESH)

    def remote(src, dst, send, recv, dev):
        return pltpu.make_async_remote_copy(src_ref=src, dst_ref=dst, send_sem=send, recv_sem=recv,
                                            device_id=dev, device_id_type=MESH)

    def same(ref, send, recv, dev):
        return remote(ref, ref, send, recv, dev)

    def landed(ref, sem):
        pltpu.make_async_copy(ref, ref, sem).wait()

    def at(start, size):
        return pl.ds(pl.multiple_of(start, size), size)

    def both(p, q, k):
        return xbuf.at[p, q // per, k, :, at(q % per * CH, CH)]

    def one(p, q, k, b):
        return xbuf.at[p, q // per, k, b, at(q % per * CH, CH)]

    def z_copy(t, q):
        rows = at((1 - part) * piece + q * CH, CH)
        return remote(yacc.at[t, rows], zr.at[t, at(q * CH, CH)], z_send.at[t, q], z_recv.at[t, q], z_dev)

    def r_copy(p, q):
        row = jnp.where(q % 2 == 0, i, y_row)
        return remote(xst.at[p, q], one(p, q, k_own, 1), r_send.at[p, q], r_recv.at[p, q], {'col': 1 - z, 'row': row})

    def y_copy(p, q, ref):
        return same(ref, y_send.at[p, q], y_recv.at[p, q], y_dev)

    def x_copy(p, q, ref):
        return same(ref, x_send.at[p, q], x_recv.at[p, q], x_dev)

    def d1_copy(p, q, ref):
        return same(ref, d1_send.at[p, q], d1_recv.at[p, q], sib_dev)

    def d2_copy(p, q):
        return same(both(p, q, k_x), d2_send.at[p, q], d2_recv.at[p, q], sib_dev)

    def s_copy(p, off):
        dev, _ = other(off)
        return remote(spart.at[p], sbuf.at[p, me], s_send.at[p, off], s_recv.at[p, me], dev)

    def send_s(p):
        sbuf[p, me] = spart[p]

        @pl.loop(1, 16)
        def _(off):
            s_copy(p, off).start()

    def sum_s(t):
        @pl.loop(1, 16)
        def _(off):
            _, dev = other(off)
            landed(sbuf.at[t, dev], s_recv.at[t, dev])

        s_sum = jnp.sum(sbuf[t].reshape(16 * 8, vecs), axis=0, keepdims=True) / vertices
        svec[...] = jnp.broadcast_to(DAMPING * s_sum + (1.0 - DAMPING), svec.shape)

    def a_start(g):
        q = lax.rem(g, blocks)
        slot = lax.rem(g, SLOTS)
        for b in range(8):
            cols = at(b * piece + q * BR, BR)
            pltpu.make_async_copy(a_ref.at[:, cols], abuf.at[slot, :, pl.ds(b * BR, BR)], a_sem.at[slot]).start()

    def a_next(g):
        @pl.when(g + SLOTS < SWEEPS * blocks)
        def _():
            a_start(g + SLOTS)

    def block_x(p, q):
        return xbuf[p, q].reshape(8 * BR, vecs)

    def multiply(p, q, g):
        slot = lax.rem(g, SLOTS)
        landed(abuf.at[slot], a_sem.at[slot])

        @pl.loop(0, 2 * piece // MT)
        def _(m):
            rows = at(m * MT, MT)
            yacc[p, rows] += jnp.dot(abuf[slot, rows], block_x(p, q), preferred_element_type=jnp.float32)

        a_next(g)

    def multiply_last(p, g):
        slot = lax.rem(g, SLOTS)
        landed(abuf.at[slot], a_sem.at[slot])
        x_last = block_x(p, blocks - 1)

        @pl.loop(0, piece // MB)
        def _(m):
            for which in (1 - part, part):
                rows = at(which * piece + m * MB, MB)
                yacc[p, rows] += jnp.dot(abuf[slot, rows], x_last, preferred_element_type=jnp.float32)

            @pl.when(m == 0)
            def _():
                for q in range(AHEAD):
                    z_copy(p, q).start()

        a_next(g)

    def clear(p):
        @pl.loop(0, 2 * piece // MB)
        def _(m):
            yacc[p, at(m * MB, MB)] = jnp.zeros((MB, vecs), jnp.float32)

    def new_rows(t, q):
        rows = at(q * CH, CH)
        landed(zr.at[t, rows], z_recv.at[t, q])
        return DAMPING * (yacc[t, at(part * piece + q * CH, CH)] + zr[t, rows]) + svec[0:1] * vperm[rows], rows

    def dang_sum(col, rows_f32):
        halves = [col * rows_f32[:, h:h + 128] for h in range(0, vecs, 128)]
        return jnp.sum(jnp.concatenate(halves, axis=1).reshape(-1, 8, vecs), axis=0)

    def dang_col(ref, b):
        return jnp.transpose(jnp.broadcast_to(ref[pl.ds(b, 1)], (BR, 128)))

    @pl.loop(0, SLOTS)
    def _(g):
        a_start(g)

    o_p = 2 * i + part
    o_dev = {'col': o_p // 8, 'row': o_p % 8}
    moves = o_p != me
    stays = o_p == me
    v_row = me // 2
    v_dev = {'col': jnp.where(me % 2 == 0, v_row // 4, 1 - v_row // 4), 'row': v_row}

    def v_copy(b):
        rows = at(b * BR, BR)
        return remote(v_ref.at[rows], vperm.at[rows], v_send.at[b], v_recv.at[b], v_dev)

    dang_copy = remote(dang_ref, dperm, dang_sem.at[0], dang_sem.at[1], v_dev)

    g_own, g_x, g_y, g_d = 2 * y + x, 2 * y + 1 - x, 2 * (1 - y) + x, 2 * (1 - y) + 1 - x
    spart[0] = jnp.zeros(spart.shape[1:], jnp.float32)

    @pl.loop(0, blocks)
    def _(b):
        rows_x = x_ref[at(b * BR, BR)]
        xbuf[0, b, g_own, c] = rows_x.astype(jnp.bfloat16)
        spart[0] += dang_sum(dang_col(dang_ref, b), rows_x)

    pl.semaphore_wait(barrier, 15)

    @pl.when(moves)
    def _():
        dang_copy.start()

    @pl.when(stays)
    def _():
        dperm[...] = dang_ref[...]
        vperm[...] = v_ref[...]

    send_s(0)
    clear(0)

    @pl.loop(0, blocks + 3 * LAG)
    def _(step):
        @pl.when(step < blocks)
        def _():
            own = xbuf.at[0, step, g_own, c]
            same(own, g_send.at[step], gx_recv.at[step], x_dev).start()
            same(own, g_send.at[step], gy_recv.at[step], y_dev).start()
            same(own, g_send.at[step], gs_recv.at[step], sib_dev).start()

        @pl.when((step >= LAG) & (step < blocks + LAG))
        def _():
            b = step - LAG
            from_x, from_y = xbuf.at[0, b, g_x, c], xbuf.at[0, b, g_y, c]
            landed(from_y, gy_recv.at[b])

            @pl.when(b % 2 == 0)
            def _():
                same(from_y, g_send.at[b], gd_recv.at[b], x_dev).start()

            landed(from_x, gx_recv.at[b])

            @pl.when(b % 2 == 1)
            def _():
                same(from_x, g_send.at[b], gd_recv.at[b], y_dev).start()

            same(from_x, g_send.at[b], gs_recv.at[b], sib_dev).start()
            same(from_y, g_send.at[b], gs_recv.at[b], sib_dev).start()

        @pl.when((step >= 2 * LAG) & (step < blocks + 2 * LAG))
        def _():
            b = step - 2 * LAG
            from_d = xbuf.at[0, b, g_d, c]
            landed(from_d, gd_recv.at[b])
            same(from_d, g_send.at[b], gs_recv.at[b], sib_dev).start()

        @pl.when(step >= 3 * LAG)
        def _():
            b = step - 3 * LAG
            landed(xbuf.at[0, b, :, 1 - c], gs_recv.at[b])

            @pl.when(b < blocks - 1)
            def _():
                multiply(0, b, b)

    @pl.when(moves)
    def _():
        for b in range(VAHEAD):
            v_copy(b).start()

    multiply_last(0, blocks - 1)

    @pl.loop(0, blocks)
    def _(b):
        landed(yacc.at[1, pl.ds(0, 7 * BR // 2)], g_send.at[b])

    @pl.loop(1, 16)
    def _(off):
        s_copy(0, off).wait_send()

    @pl.when(moves)
    def _():
        dang_copy.wait()

    @pl.loop(0, blocks)
    def _(b):
        dcol[at(b * BR, BR)] = dang_col(dperm, b)

    @pl.loop(0, SWEEPS - 1)
    def _(sweep):
        t = lax.rem(sweep, 2)
        p = 1 - t
        sum_s(t)
        clear(p)
        spart[p] = jnp.zeros(spart.shape[1:], jnp.float32)

        @pl.loop(0, chunks + 4 * LAG)
        def _(step):
            @pl.when(step + AHEAD < chunks)
            def _():
                z_copy(t, step + AHEAD).start()

            @pl.when(moves & (sweep == 0) & (step < chunks) & (step % per == 0))
            def _():
                b = step // per

                @pl.when(b + VAHEAD < blocks)
                def _():
                    v_copy(b + VAHEAD).start()

                v_copy(b).wait_recv()

            @pl.when(step < chunks)
            def _():
                q = step
                rows_new, rows = new_rows(t, q)
                rows_bf = rows_new.astype(jnp.bfloat16)

                @pl.when(home)
                def _():
                    xbuf[p, q // per, k_own, 0, at(q % per * CH, CH)] = rows_bf

                @pl.when(away)
                def _():
                    xst[p, q] = rows_bf

                spart[p] += dang_sum(dcol[rows], rows_new)

                @pl.when(away)
                def _():
                    r_copy(p, q).start()

            @pl.when(step == chunks - 1)
            def _():
                send_s(p)

            @pl.when((step >= LAG) & (step < chunks + LAG))
            def _():
                q = step - LAG
                even = q % 2 == 0

                def spread(ref):
                    y_copy(p, q, ref).start()
                    x_copy(p, q, ref).start()
                    d1_copy(p, q, ref).start()

                @pl.when(even & home)
                def _():
                    landed(one(p, q, k_own, 1), r_recv.at[p, q])
                    spread(both(p, q, k_own))

                @pl.when(jnp.logical_not(even) & away)
                def _():
                    landed(one(p, q, k_own, 1), r_recv.at[p, q])

                @pl.when(jnp.logical_not(even))
                def _():
                    spread(one(p, q, k_own, part))

            @pl.when((step >= 2 * LAG) & (step < chunks + 2 * LAG))
            def _():
                q = step - 2 * LAG
                even = q % 2 == 0

                @pl.when(even & away)
                def _():
                    ref = both(p, q, k_own)
                    landed(ref, y_recv.at[p, q])
                    x_copy(p, q, ref).start()
                    d1_copy(p, q, ref).start()

                @pl.when(jnp.logical_not(even))
                def _():
                    ref = one(p, q, k_own, 1 - part)
                    landed(ref, y_recv.at[p, q])
                    x_copy(p, q, ref).start()
                    d1_copy(p, q, ref).start()

            @pl.when((step >= 3 * LAG) & (step < chunks + 3 * LAG))
            def _():
                q = step - 3 * LAG
                landed(both(p, q, k_x), x_recv.at[p, q])
                d2_copy(p, q).start()

            @pl.when(step >= 4 * LAG)
            def _():
                q = step - 4 * LAG
                landed(both(p, q, k_sib), d1_recv.at[p, q])
                landed(both(p, q, k_d), d2_recv.at[p, q])
                b = q // per

                @pl.when((q % per == per - 1) & (b < blocks - 1))
                def _():
                    multiply(p, b, (sweep + 1) * blocks + b)

        multiply_last(p, (sweep + 1) * blocks + blocks - 1)

        @pl.loop(0, chunks)
        def _(q):
            even = q % 2 == 0
            z_copy(t, q).wait_send()
            landed(both(p, q, k_own), x_send.at[p, q])
            landed(both(p, q, k_own), d1_send.at[p, q])
            d2_copy(p, q).wait_send()

            @pl.when(even & home)
            def _():
                landed(both(p, q, k_own), y_send.at[p, q])

            @pl.when(jnp.logical_not(even))
            def _():
                landed(one(p, q, k_own, part), y_send.at[p, q])

            @pl.when(away)
            def _():
                r_copy(p, q).wait_send()

        @pl.loop(1, 16)
        def _(off):
            s_copy(p, off).wait_send()

    t = (SWEEPS - 1) % 2

    def o_copy(q):
        rows = at(q * CH, CH)
        return remote(zr.at[t, rows], o_ref.at[rows], o_send.at[q], o_recv.at[q], o_dev)

    sum_s(t)

    @pl.loop(0, chunks)
    def _(q):
        @pl.when(q + AHEAD < chunks)
        def _():
            z_copy(t, q + AHEAD).start()

        rows_new, rows = new_rows(t, q)

        @pl.when(moves)
        def _():
            zr[t, rows] = rows_new
            o_copy(q).start()

        @pl.when(stays)
        def _():
            o_ref[rows] = rows_new

    @pl.loop(0, chunks)
    def _(q):
        z_copy(t, q).wait_send()

        @pl.when(moves)
        def _():
            o_copy(q).wait()

    @pl.when(moves)
    def _():
        @pl.loop(0, blocks)
        def _(b):
            v_copy(b).wait_send()


def solution(mesh):
    def local_sweeps(mat_tile, x_piece, tele_piece, dang_piece):
        piece, vecs = x_piece.shape
        chunks, blocks = piece // CH, piece // BR
        dang_rows = dang_piece.astype(jnp.float32).reshape(blocks, 128)
        sems = pltpu.SemaphoreType.DMA
        return pl.pallas_call(
            sweeps_kernel,
            out_shape=jax.ShapeDtypeStruct((piece, vecs), jnp.float32),
            in_specs=[pl.BlockSpec(memory_space=pl.ANY)] + [pl.BlockSpec(memory_space=pltpu.VMEM)] * 3,
            out_specs=pl.BlockSpec(memory_space=pltpu.VMEM),
            scratch_shapes=[
                pltpu.VMEM((SLOTS, 2 * piece, 8 * BR), jnp.bfloat16),
                pltpu.VMEM((2, blocks, 4, 2, BR, vecs), jnp.bfloat16),
                pltpu.VMEM((2, chunks, CH, vecs), jnp.bfloat16),
                pltpu.VMEM((2, 2 * piece, vecs), jnp.float32),
                pltpu.VMEM((2, piece, vecs), jnp.float32),
                pltpu.VMEM((piece, vecs), jnp.float32),
                pltpu.VMEM((blocks, 128), jnp.float32),
                pltpu.VMEM((piece, 128), jnp.float32),
                pltpu.VMEM((2, 8, vecs), jnp.float32),
                pltpu.VMEM((2, 16, 8, vecs), jnp.float32),
                pltpu.VMEM((8, vecs), jnp.float32),
                sems((SLOTS,)),
            ] + [sems((blocks,))] * 7 + [sems((2,))] + [sems((chunks,))] * 2 + [sems((2, chunks))] * 12
            + [sems((2, 16))] * 2,
            compiler_params=pltpu.CompilerParams(collective_id=0, has_side_effects=True,
                                                 vmem_limit_bytes=67_000_000),
            name='sweeps',
        )(mat_tile, x_piece, tele_piece, dang_rows)

    vec_spec = P(('col', 'row'), None)
    return jax.shard_map(local_sweeps, mesh=mesh,
                         in_specs=(P('row', 'col'), vec_spec, vec_spec, P(('col', 'row'))),
                         out_specs=vec_spec, check_vma=False)
```

```python
import jax
import jax.numpy as jnp
from jax import lax
from jax.experimental import pallas as pl
from jax.experimental.pallas import tpu as pltpu
from jax.sharding import PartitionSpec as P

SWEEPS = 8
DAMPING = 0.85
CH = 32
BR = 128
AHEAD = 4
TAIL = 4
RELAY, BACK, BACK_RELAYED, OVER_Y, OVER_Y_RELAYED, OVER_X, OVER_X_RELAYED, HERE, HERE_RELAYED = 4, 6, 10, 10, 14, 14, 17, 16, 19
DRAIN = 17
SENT = 20
LAG = 2
FINAL_RELAY = 6
SLOTS = 3
MT = 512
MB = 256
VAHEAD = 3
MESH = pl.DeviceIdType.MESH


def sweeps_kernel(a_ref, x_ref, v_ref, dang_ref, o_ref,
                  abuf, xbuf, xst, rst, yacc, zr, vperm, dperm, dcol, spart, sbuf, svec,
                  a_sem, g_send, gx_recv, gy_recv, gd_recv, gs_recv, v_send, v_recv, dang_sem, o_send, o_recv, f_send, f_recv,
                  z_send, z_recv, r_send, r_recv, t_send, t_recv, y_send, y_recv, x_send, x_recv,
                  d1_send, d1_recv, d2_send, d2_recv, s_send, s_recv):
    i = lax.axis_index('row')
    z = lax.axis_index('col')
    y, x, c = i // 4, (i // 2) % 2, i % 2
    me = z * 8 + i
    home = z == y
    away = z != y
    part = jnp.where(home, 0, 1)
    k_own = 2 * x + c
    k_sib = 2 * x + 1 - c
    k_x = 2 * (1 - x) + c
    k_d = 2 * (1 - x) + 1 - c
    sib_dev = {'col': z, 'row': i + 1 - 2 * c}
    x_dev = {'col': z, 'row': i + 2 - 4 * x}
    y_row = i + 4 - 8 * y
    y_dev = {'col': z, 'row': y_row}
    z_dev = {'col': 1 - z, 'row': i}
    piece, vecs = o_ref.shape
    chunks = piece // CH
    blocks = piece // BR
    per = BR // CH
    vertices = 16 * piece

    def other(off):
        dev = (me + off) % 16
        return {'col': dev // 8, 'row': dev % 8}, dev

    barrier = pltpu.get_barrier_semaphore()

    @pl.loop(1, 16)
    def _(off):
        dev, _ = other(off)
        pl.semaphore_signal(barrier, inc=1, device_id=dev, device_id_type=MESH)

    def remote(src, dst, send, recv, dev):
        return pltpu.make_async_remote_copy(src_ref=src, dst_ref=dst, send_sem=send, recv_sem=recv,
                                            device_id=dev, device_id_type=MESH)

    def same(ref, send, recv, dev):
        return remote(ref, ref, send, recv, dev)

    def landed(ref, sem):
        pltpu.make_async_copy(ref, ref, sem).wait()

    def at(start, size):
        return pl.ds(pl.multiple_of(start, size), size)

    def both(p, q, k):
        return xbuf.at[p, q // per, k, :, at(q % per * CH, CH)]

    def one(p, q, k, b):
        return xbuf.at[p, q // per, k, b, at(q % per * CH, CH)]

    def z_copy(t, q):
        rows = at((1 - part) * piece + q * CH, CH)
        return remote(yacc.at[t, rows], zr.at[t, at(q * CH, CH)], z_send.at[t, q], z_recv.at[t, q], z_dev)

    def relayed(q):
        return (q % 2 == 0) & (q < chunks - TAIL)

    def direct(q):
        return jnp.logical_not(relayed(q))

    def r_copy(p, q):
        return remote(xst.at[p, q], one(p, q, k_own, 1), r_send.at[p, q], r_recv.at[p, q], z_dev)

    def to_relay(p, q):
        return remote(xst.at[p, q], rst.at[p, q // 2], r_send.at[p, q], t_recv.at[p, q // 2], y_dev)

    def from_relay(p, q):
        return remote(rst.at[p, q // 2], one(p, q, k_own, 1), t_send.at[p, q // 2], r_recv.at[p, q], z_dev)

    def y_copy(p, q, ref):
        return same(ref, y_send.at[p, q], y_recv.at[p, q], y_dev)

    def x_copy(p, q, ref):
        return same(ref, x_send.at[p, q], x_recv.at[p, q], x_dev)

    def d1_copy(p, q, ref):
        return same(ref, d1_send.at[p, q], d1_recv.at[p, q], sib_dev)

    def d2_copy(p, q):
        return same(both(p, q, k_x), d2_send.at[p, q], d2_recv.at[p, q], sib_dev)

    def s_copy(p, off):
        dev, _ = other(off)
        return remote(spart.at[p], sbuf.at[p, me], s_send.at[p, off], s_recv.at[p, me], dev)

    def send_s(p):
        sbuf[p, me] = spart[p]

        @pl.loop(1, 16)
        def _(off):
            s_copy(p, off).start()

    def sum_s(t):
        @pl.loop(1, 16)
        def _(off):
            _, dev = other(off)
            landed(sbuf.at[t, dev], s_recv.at[t, dev])

        s_sum = jnp.sum(sbuf[t].reshape(16 * 8, vecs), axis=0, keepdims=True) / vertices
        svec[...] = jnp.broadcast_to(DAMPING * s_sum + (1.0 - DAMPING), svec.shape)

    def a_start(g):
        q = lax.rem(g, blocks)
        slot = lax.rem(g, SLOTS)
        for b in range(8):
            cols = at(b * piece + q * BR, BR)
            pltpu.make_async_copy(a_ref.at[:, cols], abuf.at[slot, :, pl.ds(b * BR, BR)], a_sem.at[slot]).start()

    def a_next(g):
        @pl.when(g + SLOTS < SWEEPS * blocks)
        def _():
            a_start(g + SLOTS)

    def block_x(p, q):
        return xbuf[p, q].reshape(8 * BR, vecs)

    def multiply(p, b, g, k):
        slot = lax.rem(g, SLOTS)

        @pl.when(k == 0)
        def _():
            landed(abuf.at[slot], a_sem.at[slot])

        x_k = xbuf[p, b, k].reshape(2 * BR, vecs)

        @pl.loop(0, 2 * piece // MT)
        def _(m):
            rows = at(m * MT, MT)
            yacc[p, rows] += jnp.dot(abuf[slot, rows, at(k * 2 * BR, 2 * BR)], x_k, preferred_element_type=jnp.float32)

        @pl.when(k == 3)
        def _():
            a_next(g)

    def multiply_last(p, g):
        slot = lax.rem(g, SLOTS)
        landed(abuf.at[slot], a_sem.at[slot])
        x_last = block_x(p, blocks - 1)

        @pl.loop(0, piece // MB)
        def _(m):
            for which in (1 - part, part):
                rows = at(which * piece + m * MB, MB)
                yacc[p, rows] += jnp.dot(abuf[slot, rows], x_last, preferred_element_type=jnp.float32)

            @pl.when(m == 0)
            def _():
                for q in range(AHEAD):
                    z_copy(p, q).start()

        a_next(g)

    def clear(p):
        @pl.loop(0, 2 * piece // MB)
        def _(m):
            yacc[p, at(m * MB, MB)] = jnp.zeros((MB, vecs), jnp.float32)

    def new_rows(t, q):
        rows = at(q * CH, CH)
        landed(zr.at[t, rows], z_recv.at[t, q])
        return DAMPING * (yacc[t, at(part * piece + q * CH, CH)] + zr[t, rows]) + svec[0:1] * vperm[rows], rows

    def dang_sum(col, rows_f32):
        halves = [col * rows_f32[:, h:h + 128] for h in range(0, vecs, 128)]
        return jnp.sum(jnp.concatenate(halves, axis=1).reshape(-1, 8, vecs), axis=0)

    def dang_col(ref, b):
        return jnp.transpose(jnp.broadcast_to(ref[pl.ds(b, 1)], (BR, 128)))

    @pl.loop(0, SLOTS)
    def _(g):
        a_start(g)

    o_p = 2 * i + part
    o_dev = {'col': o_p // 8, 'row': o_p % 8}
    moves = o_p != me
    stays = o_p == me
    v_row = me // 2
    v_dev = {'col': jnp.where(me % 2 == 0, v_row // 4, 1 - v_row // 4), 'row': v_row}

    def v_copy(b):
        rows = at(b * BR, BR)
        return remote(v_ref.at[rows], vperm.at[rows], v_send.at[b], v_recv.at[b], v_dev)

    dang_copy = remote(dang_ref, dperm, dang_sem.at[0], dang_sem.at[1], v_dev)

    g_own, g_x, g_y, g_d = 2 * y + x, 2 * y + 1 - x, 2 * (1 - y) + x, 2 * (1 - y) + 1 - x
    spart[0] = jnp.zeros(spart.shape[1:], jnp.float32)

    @pl.loop(0, blocks)
    def _(b):
        rows_x = x_ref[at(b * BR, BR)]
        xbuf[0, b, g_own, c] = rows_x.astype(jnp.bfloat16)
        spart[0] += dang_sum(dang_col(dang_ref, b), rows_x)

    pl.semaphore_wait(barrier, 15)

    @pl.when(moves)
    def _():
        dang_copy.start()

    @pl.when(stays)
    def _():
        dperm[...] = dang_ref[...]
        vperm[...] = v_ref[...]

    send_s(0)
    clear(0)

    @pl.loop(0, blocks + 3 * LAG)
    def _(step):
        @pl.when(step < blocks)
        def _():
            own = xbuf.at[0, step, g_own, c]
            same(own, g_send.at[step], gx_recv.at[step], x_dev).start()
            same(own, g_send.at[step], gy_recv.at[step], y_dev).start()
            same(own, g_send.at[step], gs_recv.at[step], sib_dev).start()

        @pl.when((step >= LAG) & (step < blocks + LAG))
        def _():
            b = step - LAG
            from_x, from_y = xbuf.at[0, b, g_x, c], xbuf.at[0, b, g_y, c]
            landed(from_y, gy_recv.at[b])

            @pl.when(b % 2 == 0)
            def _():
                same(from_y, g_send.at[b], gd_recv.at[b], x_dev).start()

            landed(from_x, gx_recv.at[b])

            @pl.when(b % 2 == 1)
            def _():
                same(from_x, g_send.at[b], gd_recv.at[b], y_dev).start()

            same(from_x, g_send.at[b], gs_recv.at[b], sib_dev).start()
            same(from_y, g_send.at[b], gs_recv.at[b], sib_dev).start()

        @pl.when((step >= 2 * LAG) & (step < blocks + 2 * LAG))
        def _():
            b = step - 2 * LAG
            from_d = xbuf.at[0, b, g_d, c]
            landed(from_d, gd_recv.at[b])
            same(from_d, g_send.at[b], gs_recv.at[b], sib_dev).start()

        @pl.when(step >= 3 * LAG)
        def _():
            b = step - 3 * LAG
            landed(xbuf.at[0, b, :, 1 - c], gs_recv.at[b])

            @pl.when(b < blocks - 1)
            def _():
                for k in range(4):
                    multiply(0, b, b, k)

    @pl.when(moves)
    def _():
        for b in range(VAHEAD):
            v_copy(b).start()

    multiply_last(0, blocks - 1)

    @pl.loop(0, blocks)
    def _(b):
        landed(yacc.at[1, pl.ds(0, 7 * BR // 2)], g_send.at[b])

    @pl.loop(1, 16)
    def _(off):
        s_copy(0, off).wait_send()

    @pl.when(moves)
    def _():
        dang_copy.wait()

    @pl.loop(0, blocks)
    def _(b):
        dcol[at(b * BR, BR)] = dang_col(dperm, b)

    @pl.loop(0, SWEEPS - 1)
    def _(sweep):
        t = lax.rem(sweep, 2)
        p = 1 - t
        sum_s(t)
        spart[p] = jnp.zeros(spart.shape[1:], jnp.float32)

        def spread(q, ref):
            y_copy(p, q, ref).start()
            x_copy(p, q, ref).start()
            d1_copy(p, q, ref).start()

        def forward(q, ref):
            landed(ref, y_recv.at[p, q])
            x_copy(p, q, ref).start()
            d1_copy(p, q, ref).start()

        def sent(q):
            z_copy(t, q).wait_send()
            landed(both(p, q, k_own), x_send.at[p, q])
            landed(both(p, q, k_own), d1_send.at[p, q])
            d2_copy(p, q).wait_send()

            @pl.when(away)
            def _():
                r_copy(p, q).wait_send()

            @pl.when(direct(q) & home)
            def _():
                landed(both(p, q, k_own), y_send.at[p, q])

            @pl.when(relayed(q))
            def _():
                landed(one(p, q, k_own, part), y_send.at[p, q])

            @pl.when(relayed(q) & home)
            def _():
                from_relay(p, q).wait_send()

        @pl.loop(0, chunks + DRAIN)
        def _(step):
            def chunk(lag, where):
                q = step - lag
                return q, (q >= 0) & (q < chunks) & where(q)

            @pl.when(step + AHEAD < chunks)
            def _():
                z_copy(t, step + AHEAD).start()

            @pl.when(moves & (sweep == 0) & (step < chunks) & (step % per == 0))
            def _():
                b = step // per

                @pl.when(b + VAHEAD < blocks)
                def _():
                    v_copy(b + VAHEAD).start()

                v_copy(b).wait_recv()

            @pl.when(step < chunks)
            def _():
                q = step
                rows_new, rows = new_rows(t, q)
                rows_bf = rows_new.astype(jnp.bfloat16)

                @pl.when(home)
                def _():
                    xbuf[p, q // per, k_own, 0, at(q % per * CH, CH)] = rows_bf

                @pl.when(away)
                def _():
                    xst[p, q] = rows_bf

                spart[p] += dang_sum(dcol[rows], rows_new)

                @pl.when(away & relayed(q))
                def _():
                    to_relay(p, q).start()

                @pl.when(away & direct(q))
                def _():
                    r_copy(p, q).start()

            @pl.when(step == chunks - 1)
            def _():
                send_s(p)

            q, on = chunk(RELAY, relayed)

            @pl.when(on & home)
            def _():
                landed(rst.at[p, q // 2], t_recv.at[p, q // 2])
                from_relay(p, q).start()
                spread(q, one(p, q, k_own, 0))

            q, on = chunk(BACK, direct)

            @pl.when(on & home)
            def _():
                landed(one(p, q, k_own, 1), r_recv.at[p, q])
                spread(q, both(p, q, k_own))

            q, on = chunk(OVER_Y, direct)

            @pl.when(on & away)
            def _():
                forward(q, both(p, q, k_own))

            q, on = chunk(BACK_RELAYED, relayed)

            @pl.when(on & away)
            def _():
                forward(q, one(p, q, k_own, 0))
                landed(one(p, q, k_own, 1), r_recv.at[p, q])
                spread(q, one(p, q, k_own, 1))

            q, on = chunk(OVER_Y_RELAYED, relayed)

            @pl.when(on & home)
            def _():
                forward(q, one(p, q, k_own, 1))

            for lag, where in ((OVER_X, direct), (OVER_X_RELAYED, relayed)):
                q, on = chunk(lag, where)

                @pl.when(on)
                def _(q=q):
                    landed(both(p, q, k_x), x_recv.at[p, q])
                    d2_copy(p, q).start()

            for lag, where in ((HERE, direct), (HERE_RELAYED, relayed)):
                q, on = chunk(lag, where)

                @pl.when(on)
                def _(q=q):
                    landed(both(p, q, k_sib), d1_recv.at[p, q])
                    landed(both(p, q, k_d), d2_recv.at[p, q])

            @pl.when(step == per)
            def _():
                clear(p)

            turn = step - HERE_RELAYED - per // 2
            b = turn // per

            @pl.when((turn >= 0) & (b < blocks - 1))
            def _():
                for k in range(4 // per):
                    multiply(p, b, (sweep + 1) * blocks + b, turn % per * (4 // per) + k)

            q, on = chunk(SENT, lambda q: True)

            @pl.when(on)
            def _():
                sent(q)

        multiply_last(p, (sweep + 1) * blocks + blocks - 1)

        @pl.loop(chunks + DRAIN - SENT, chunks)
        def _(q):
            sent(q)

        @pl.loop(1, 16)
        def _(off):
            s_copy(p, off).wait_send()

    t = (SWEEPS - 1) % 2

    def o_copy(q):
        rows = at(q * CH, CH)
        return remote(zr.at[t, rows], o_ref.at[rows], o_send.at[q], o_recv.at[q], o_dev)

    def o_to_relay(q):
        rows = at(q * CH, CH)
        return remote(zr.at[t, rows], zr.at[1 - t, rows], o_send.at[q], f_recv.at[q], y_dev)

    def o_from_relay(q):
        rows = at(q * CH, CH)
        dev = 2 * y_row + 1
        return remote(zr.at[1 - t, rows], o_ref.at[rows], f_send.at[q], o_recv.at[q],
                      {'col': dev // 8, 'row': dev % 8})

    sum_s(t)

    @pl.loop(0, chunks + FINAL_RELAY)
    def _(step):
        @pl.when(step + AHEAD < chunks)
        def _():
            z_copy(t, step + AHEAD).start()

        @pl.when(step < chunks)
        def _():
            rows_new, rows = new_rows(t, step)

            @pl.when(moves)
            def _():
                zr[t, rows] = rows_new

            @pl.when(away & relayed(step))
            def _():
                o_to_relay(step).start()

            @pl.when(moves & (home | direct(step)))
            def _():
                o_copy(step).start()

            @pl.when(stays)
            def _():
                o_ref[rows] = rows_new

        q = step - FINAL_RELAY

        @pl.when((q >= 0) & relayed(q) & home)
        def _():
            rows = at(q * CH, CH)
            landed(zr.at[1 - t, rows], f_recv.at[q])
            o_from_relay(q).start()

    @pl.loop(0, chunks)
    def _(q):
        z_copy(t, q).wait_send()

        @pl.when(moves)
        def _():
            o_copy(q).wait()

        @pl.when(relayed(q) & home)
        def _():
            o_from_relay(q).wait_send()

    @pl.when(moves)
    def _():
        @pl.loop(0, blocks)
        def _(b):
            v_copy(b).wait_send()


def solution(mesh):
    def local_sweeps(mat_tile, x_piece, tele_piece, dang_piece):
        piece, vecs = x_piece.shape
        chunks, blocks = piece // CH, piece // BR
        dang_rows = dang_piece.astype(jnp.float32).reshape(blocks, 128)
        sems = pltpu.SemaphoreType.DMA
        return pl.pallas_call(
            sweeps_kernel,
            out_shape=jax.ShapeDtypeStruct((piece, vecs), jnp.float32),
            in_specs=[pl.BlockSpec(memory_space=pl.ANY)] + [pl.BlockSpec(memory_space=pltpu.VMEM)] * 3,
            out_specs=pl.BlockSpec(memory_space=pltpu.VMEM),
            scratch_shapes=[
                pltpu.VMEM((SLOTS, 2 * piece, 8 * BR), jnp.bfloat16),
                pltpu.VMEM((2, blocks, 4, 2, BR, vecs), jnp.bfloat16),
                pltpu.VMEM((2, chunks, CH, vecs), jnp.bfloat16),
                pltpu.VMEM((2, chunks // 2, CH, vecs), jnp.bfloat16),
                pltpu.VMEM((2, 2 * piece, vecs), jnp.float32),
                pltpu.VMEM((2, piece, vecs), jnp.float32),
                pltpu.VMEM((piece, vecs), jnp.float32),
                pltpu.VMEM((blocks, 128), jnp.float32),
                pltpu.VMEM((piece, 128), jnp.float32),
                pltpu.VMEM((2, 8, vecs), jnp.float32),
                pltpu.VMEM((2, 16, 8, vecs), jnp.float32),
                pltpu.VMEM((8, vecs), jnp.float32),
                sems((SLOTS,)),
            ] + [sems((blocks,))] * 7 + [sems((2,))] + [sems((chunks,))] * 4 + [sems((2, chunks))] * 4
            + [sems((2, chunks // 2))] * 2 + [sems((2, chunks))] * 8
            + [sems((2, 16))] * 2,
            compiler_params=pltpu.CompilerParams(collective_id=0, has_side_effects=True,
                                                 vmem_limit_bytes=67_000_000),
            name='sweeps',
        )(mat_tile, x_piece, tele_piece, dang_rows)

    vec_spec = P(('col', 'row'), None)
    return jax.shard_map(local_sweeps, mesh=mesh,
                         in_specs=(P('row', 'col'), vec_spec, vec_spec, P(('col', 'row'))),
                         out_specs=vec_spec, check_vma=False)
```

```python
import jax
import jax.numpy as jnp
from jax import lax
from jax.experimental import pallas as pl
from jax.experimental.pallas import tpu as pltpu
from jax.sharding import PartitionSpec as P

SWEEPS = 8
DAMPING = 0.85
CH = 64
BR = 128
AHEAD = 3
TAIL = 2
RELAY, BACK, BACK_RELAYED, OVER_Y, OVER_Y_RELAYED, OVER_X, OVER_X_RELAYED, HERE, HERE_RELAYED = 2, 3, 5, 5, 7, 7, 9, 8, 10
DRAIN = 8
SENT = 11
LAG = 2
FINAL_RELAY = 3
SLOTS = 3
MT = 512
MB = 256
VAHEAD = 3
MESH = pl.DeviceIdType.MESH


def sweeps_kernel(a_ref, x_ref, v_ref, dang_ref, o_ref,
                  abuf, xbuf, xst, rst, yacc, zr, vperm, dperm, dcol, spart, sbuf, svec,
                  a_sem, g_send, gx_recv, gy_recv, gd_recv, gs_recv, v_send, v_recv, dang_sem, o_send, o_recv, f_send, f_recv,
                  z_send, z_recv, r_send, r_recv, t_send, t_recv, y_send, y_recv, x_send, x_recv,
                  d1_send, d1_recv, d2_send, d2_recv, s_send, s_recv):
    i = lax.axis_index('row')
    z = lax.axis_index('col')
    y, x, c = i // 4, (i // 2) % 2, i % 2
    me = z * 8 + i
    home = z == y
    away = z != y
    part = jnp.where(home, 0, 1)
    k_own = 2 * x + c
    k_sib = 2 * x + 1 - c
    k_x = 2 * (1 - x) + c
    k_d = 2 * (1 - x) + 1 - c
    sib_dev = {'col': z, 'row': i + 1 - 2 * c}
    x_dev = {'col': z, 'row': i + 2 - 4 * x}
    y_row = i + 4 - 8 * y
    y_dev = {'col': z, 'row': y_row}
    z_dev = {'col': 1 - z, 'row': i}
    piece, vecs = o_ref.shape
    chunks = piece // CH
    blocks = piece // BR
    per = BR // CH
    vertices = 16 * piece

    def other(off):
        dev = (me + off) % 16
        return {'col': dev // 8, 'row': dev % 8}, dev

    barrier = pltpu.get_barrier_semaphore()

    @pl.loop(1, 16)
    def _(off):
        dev, _ = other(off)
        pl.semaphore_signal(barrier, inc=1, device_id=dev, device_id_type=MESH)

    def remote(src, dst, send, recv, dev):
        return pltpu.make_async_remote_copy(src_ref=src, dst_ref=dst, send_sem=send, recv_sem=recv,
                                            device_id=dev, device_id_type=MESH)

    def same(ref, send, recv, dev):
        return remote(ref, ref, send, recv, dev)

    def landed(ref, sem):
        pltpu.make_async_copy(ref, ref, sem).wait()

    def at(start, size):
        return pl.ds(pl.multiple_of(start, size), size)

    def both(p, q, k):
        return xbuf.at[p, q // per, k, :, at(q % per * CH, CH)]

    def one(p, q, k, b):
        return xbuf.at[p, q // per, k, b, at(q % per * CH, CH)]

    def z_copy(t, q):
        rows = at((1 - part) * piece + q * CH, CH)
        return remote(yacc.at[t, rows], zr.at[t, at(q * CH, CH)], z_send.at[t, q], z_recv.at[t, q], z_dev)

    def relayed(q):
        return (q % 2 == 0) & (q < chunks - TAIL)

    def direct(q):
        return jnp.logical_not(relayed(q))

    def r_copy(p, q):
        return remote(xst.at[p, q], one(p, q, k_own, 1), r_send.at[p, q], r_recv.at[p, q], z_dev)

    def to_relay(p, q):
        return remote(xst.at[p, q], rst.at[p, q // 2], r_send.at[p, q], t_recv.at[p, q // 2], y_dev)

    def from_relay(p, q):
        return remote(rst.at[p, q // 2], one(p, q, k_own, 1), t_send.at[p, q // 2], r_recv.at[p, q], z_dev)

    def y_copy(p, q, ref):
        return same(ref, y_send.at[p, q], y_recv.at[p, q], y_dev)

    def x_copy(p, q, ref):
        return same(ref, x_send.at[p, q], x_recv.at[p, q], x_dev)

    def d1_copy(p, q, ref):
        return same(ref, d1_send.at[p, q], d1_recv.at[p, q], sib_dev)

    def d2_copy(p, q):
        return same(both(p, q, k_x), d2_send.at[p, q], d2_recv.at[p, q], sib_dev)

    def s_copy(p, off):
        dev, _ = other(off)
        return remote(spart.at[p], sbuf.at[p, me], s_send.at[p, off], s_recv.at[p, me], dev)

    def send_s(p):
        sbuf[p, me] = spart[p]

        @pl.loop(1, 16)
        def _(off):
            s_copy(p, off).start()

    def sum_s(t):
        @pl.loop(1, 16)
        def _(off):
            _, dev = other(off)
            landed(sbuf.at[t, dev], s_recv.at[t, dev])

        s_sum = jnp.sum(sbuf[t].reshape(16 * 8, vecs), axis=0, keepdims=True) / vertices
        svec[...] = jnp.broadcast_to(DAMPING * s_sum + (1.0 - DAMPING), svec.shape)

    def a_start(g):
        q = lax.rem(g, blocks)
        slot = lax.rem(g, SLOTS)
        for b in range(8):
            cols = at(b * piece + q * BR, BR)
            pltpu.make_async_copy(a_ref.at[:, cols], abuf.at[slot, :, pl.ds(b * BR, BR)], a_sem.at[slot]).start()

    def a_next(g):
        @pl.when(g + SLOTS < SWEEPS * blocks)
        def _():
            a_start(g + SLOTS)

    def block_x(p, q):
        return xbuf[p, q].reshape(8 * BR, vecs)

    def multiply(p, b, g, turn):
        slot = lax.rem(g, SLOTS)
        share = 2 * piece // per

        @pl.when(turn == 0)
        def _():
            landed(abuf.at[slot], a_sem.at[slot])

        @pl.loop(0, share // MT)
        def _(m):
            rows = at(turn * share + m * MT, MT)
            yacc[p, rows] += jnp.dot(abuf[slot, rows], block_x(p, b), preferred_element_type=jnp.float32)

        @pl.when(turn == per - 1)
        def _():
            a_next(g)

    def multiply_last(p, g):
        slot = lax.rem(g, SLOTS)
        landed(abuf.at[slot], a_sem.at[slot])
        x_last = block_x(p, blocks - 1)

        @pl.loop(0, piece // MB)
        def _(m):
            for which in (1 - part, part):
                rows = at(which * piece + m * MB, MB)
                yacc[p, rows] += jnp.dot(abuf[slot, rows], x_last, preferred_element_type=jnp.float32)

            @pl.when(m == 0)
            def _():
                for q in range(AHEAD):
                    z_copy(p, q).start()

        a_next(g)

    def clear(p):
        @pl.loop(0, 2 * piece // MB)
        def _(m):
            yacc[p, at(m * MB, MB)] = jnp.zeros((MB, vecs), jnp.float32)

    def new_rows(t, q):
        rows = at(q * CH, CH)
        landed(zr.at[t, rows], z_recv.at[t, q])
        return DAMPING * (yacc[t, at(part * piece + q * CH, CH)] + zr[t, rows]) + svec[0:1] * vperm[rows], rows

    def dang_sum(col, rows_f32):
        halves = [col * rows_f32[:, h:h + 128] for h in range(0, vecs, 128)]
        return jnp.sum(jnp.concatenate(halves, axis=1).reshape(-1, 8, vecs), axis=0)

    def dang_col(ref, b):
        return jnp.transpose(jnp.broadcast_to(ref[pl.ds(b, 1)], (BR, 128)))

    @pl.loop(0, SLOTS)
    def _(g):
        a_start(g)

    o_p = 2 * i + part
    o_dev = {'col': o_p // 8, 'row': o_p % 8}
    moves = o_p != me
    stays = o_p == me
    v_row = me // 2
    v_dev = {'col': jnp.where(me % 2 == 0, v_row // 4, 1 - v_row // 4), 'row': v_row}

    def v_copy(b):
        rows = at(b * BR, BR)
        return remote(v_ref.at[rows], vperm.at[rows], v_send.at[b], v_recv.at[b], v_dev)

    dang_copy = remote(dang_ref, dperm, dang_sem.at[0], dang_sem.at[1], v_dev)

    g_own, g_x, g_y, g_d = 2 * y + x, 2 * y + 1 - x, 2 * (1 - y) + x, 2 * (1 - y) + 1 - x
    spart[0] = jnp.zeros(spart.shape[1:], jnp.float32)

    @pl.loop(0, blocks)
    def _(b):
        rows_x = x_ref[at(b * BR, BR)]
        xbuf[0, b, g_own, c] = rows_x.astype(jnp.bfloat16)
        spart[0] += dang_sum(dang_col(dang_ref, b), rows_x)

    pl.semaphore_wait(barrier, 15)

    @pl.when(moves)
    def _():
        dang_copy.start()

    @pl.when(stays)
    def _():
        dperm[...] = dang_ref[...]
        vperm[...] = v_ref[...]

    send_s(0)
    clear(0)

    @pl.loop(0, blocks + 3 * LAG)
    def _(step):
        @pl.when(step < blocks)
        def _():
            own = xbuf.at[0, step, g_own, c]
            same(own, g_send.at[step], gx_recv.at[step], x_dev).start()
            same(own, g_send.at[step], gy_recv.at[step], y_dev).start()
            same(own, g_send.at[step], gs_recv.at[step], sib_dev).start()

        @pl.when((step >= LAG) & (step < blocks + LAG))
        def _():
            b = step - LAG
            from_x, from_y = xbuf.at[0, b, g_x, c], xbuf.at[0, b, g_y, c]
            landed(from_y, gy_recv.at[b])

            @pl.when(b % 2 == 0)
            def _():
                same(from_y, g_send.at[b], gd_recv.at[b], x_dev).start()

            landed(from_x, gx_recv.at[b])

            @pl.when(b % 2 == 1)
            def _():
                same(from_x, g_send.at[b], gd_recv.at[b], y_dev).start()

            same(from_x, g_send.at[b], gs_recv.at[b], sib_dev).start()
            same(from_y, g_send.at[b], gs_recv.at[b], sib_dev).start()

        @pl.when((step >= 2 * LAG) & (step < blocks + 2 * LAG))
        def _():
            b = step - 2 * LAG
            from_d = xbuf.at[0, b, g_d, c]
            landed(from_d, gd_recv.at[b])
            same(from_d, g_send.at[b], gs_recv.at[b], sib_dev).start()

        @pl.when(step >= 3 * LAG)
        def _():
            b = step - 3 * LAG
            landed(xbuf.at[0, b, :, 1 - c], gs_recv.at[b])

            @pl.when(b < blocks - 1)
            def _():
                @pl.loop(0, per)
                def _(turn):
                    multiply(0, b, b, turn)

    @pl.when(moves)
    def _():
        for b in range(VAHEAD):
            v_copy(b).start()

    multiply_last(0, blocks - 1)

    @pl.loop(0, blocks)
    def _(b):
        landed(yacc.at[1, pl.ds(0, 7 * BR // 2)], g_send.at[b])

    @pl.loop(1, 16)
    def _(off):
        s_copy(0, off).wait_send()

    @pl.when(moves)
    def _():
        dang_copy.wait()

    @pl.loop(0, blocks)
    def _(b):
        dcol[at(b * BR, BR)] = dang_col(dperm, b)

    @pl.loop(0, SWEEPS - 1)
    def _(sweep):
        t = lax.rem(sweep, 2)
        p = 1 - t
        sum_s(t)
        spart[p] = jnp.zeros(spart.shape[1:], jnp.float32)

        def spread(q, ref):
            y_copy(p, q, ref).start()
            x_copy(p, q, ref).start()
            d1_copy(p, q, ref).start()

        def forward(q, ref):
            landed(ref, y_recv.at[p, q])
            x_copy(p, q, ref).start()
            d1_copy(p, q, ref).start()

        def sent(q):
            z_copy(t, q).wait_send()
            landed(both(p, q, k_own), x_send.at[p, q])
            landed(both(p, q, k_own), d1_send.at[p, q])
            d2_copy(p, q).wait_send()

            @pl.when(away)
            def _():
                r_copy(p, q).wait_send()

            @pl.when(direct(q) & home)
            def _():
                landed(both(p, q, k_own), y_send.at[p, q])

            @pl.when(relayed(q))
            def _():
                landed(one(p, q, k_own, part), y_send.at[p, q])

            @pl.when(relayed(q) & home)
            def _():
                from_relay(p, q).wait_send()

        @pl.loop(0, chunks + DRAIN)
        def _(step):
            def chunk(lag, where):
                q = step - lag
                return q, (q >= 0) & (q < chunks) & where(q)

            @pl.when(step + AHEAD < chunks)
            def _():
                z_copy(t, step + AHEAD).start()

            @pl.when(moves & (sweep == 0) & (step < chunks) & (step % per == 0))
            def _():
                b = step // per

                @pl.when(b + VAHEAD < blocks)
                def _():
                    v_copy(b + VAHEAD).start()

                v_copy(b).wait_recv()

            @pl.when(step < chunks)
            def _():
                q = step
                rows_new, rows = new_rows(t, q)
                rows_bf = rows_new.astype(jnp.bfloat16)

                @pl.when(home)
                def _():
                    xbuf[p, q // per, k_own, 0, at(q % per * CH, CH)] = rows_bf

                @pl.when(away)
                def _():
                    xst[p, q] = rows_bf

                spart[p] += dang_sum(dcol[rows], rows_new)

                @pl.when(away & relayed(q))
                def _():
                    to_relay(p, q).start()

                @pl.when(away & direct(q))
                def _():
                    r_copy(p, q).start()

            @pl.when(step == chunks - 1)
            def _():
                send_s(p)

            q, on = chunk(RELAY, relayed)

            @pl.when(on & home)
            def _():
                landed(rst.at[p, q // 2], t_recv.at[p, q // 2])
                from_relay(p, q).start()
                spread(q, one(p, q, k_own, 0))

            q, on = chunk(BACK, direct)

            @pl.when(on & home)
            def _():
                landed(one(p, q, k_own, 1), r_recv.at[p, q])
                spread(q, both(p, q, k_own))

            q, on = chunk(OVER_Y, direct)

            @pl.when(on & away)
            def _():
                forward(q, both(p, q, k_own))

            q, on = chunk(BACK_RELAYED, relayed)

            @pl.when(on & away)
            def _():
                forward(q, one(p, q, k_own, 0))
                landed(one(p, q, k_own, 1), r_recv.at[p, q])
                spread(q, one(p, q, k_own, 1))

            q, on = chunk(OVER_Y_RELAYED, relayed)

            @pl.when(on & home)
            def _():
                forward(q, one(p, q, k_own, 1))

            for lag, where in ((OVER_X, direct), (OVER_X_RELAYED, relayed)):
                q, on = chunk(lag, where)

                @pl.when(on)
                def _(q=q):
                    landed(both(p, q, k_x), x_recv.at[p, q])
                    d2_copy(p, q).start()

            for lag, where in ((HERE, direct), (HERE_RELAYED, relayed)):
                q, on = chunk(lag, where)

                @pl.when(on)
                def _(q=q):
                    landed(both(p, q, k_sib), d1_recv.at[p, q])
                    landed(both(p, q, k_d), d2_recv.at[p, q])

            @pl.when(step == per)
            def _():
                clear(p)

            turn = step - HERE_RELAYED
            b = turn // per

            @pl.when((turn >= 0) & (b < blocks - 1))
            def _():
                multiply(p, b, (sweep + 1) * blocks + b, turn % per)

            q, on = chunk(SENT, lambda q: True)

            @pl.when(on)
            def _():
                sent(q)

        multiply_last(p, (sweep + 1) * blocks + blocks - 1)

        @pl.loop(chunks + DRAIN - SENT, chunks)
        def _(q):
            sent(q)

        @pl.loop(1, 16)
        def _(off):
            s_copy(p, off).wait_send()

    t = (SWEEPS - 1) % 2

    def o_copy(q):
        rows = at(q * CH, CH)
        return remote(zr.at[t, rows], o_ref.at[rows], o_send.at[q], o_recv.at[q], o_dev)

    def o_to_relay(q):
        rows = at(q * CH, CH)
        return remote(zr.at[t, rows], zr.at[1 - t, rows], o_send.at[q], f_recv.at[q], y_dev)

    def o_from_relay(q):
        rows = at(q * CH, CH)
        dev = 2 * y_row + 1
        return remote(zr.at[1 - t, rows], o_ref.at[rows], f_send.at[q], o_recv.at[q],
                      {'col': dev // 8, 'row': dev % 8})

    sum_s(t)

    @pl.loop(0, chunks + FINAL_RELAY)
    def _(step):
        @pl.when(step + AHEAD < chunks)
        def _():
            z_copy(t, step + AHEAD).start()

        @pl.when(step < chunks)
        def _():
            rows_new, rows = new_rows(t, step)

            @pl.when(moves)
            def _():
                zr[t, rows] = rows_new

            @pl.when(away & relayed(step))
            def _():
                o_to_relay(step).start()

            @pl.when(moves & (home | direct(step)))
            def _():
                o_copy(step).start()

            @pl.when(stays)
            def _():
                o_ref[rows] = rows_new

        q = step - FINAL_RELAY

        @pl.when((q >= 0) & relayed(q) & home)
        def _():
            rows = at(q * CH, CH)
            landed(zr.at[1 - t, rows], f_recv.at[q])
            o_from_relay(q).start()

    @pl.loop(0, chunks)
    def _(q):
        z_copy(t, q).wait_send()

        @pl.when(moves)
        def _():
            o_copy(q).wait()

        @pl.when(relayed(q) & home)
        def _():
            o_from_relay(q).wait_send()

    @pl.when(moves)
    def _():
        @pl.loop(0, blocks)
        def _(b):
            v_copy(b).wait_send()


def solution(mesh):
    def local_sweeps(mat_tile, x_piece, tele_piece, dang_piece):
        piece, vecs = x_piece.shape
        chunks, blocks = piece // CH, piece // BR
        dang_rows = dang_piece.astype(jnp.float32).reshape(blocks, 128)
        sems = pltpu.SemaphoreType.DMA
        return pl.pallas_call(
            sweeps_kernel,
            out_shape=jax.ShapeDtypeStruct((piece, vecs), jnp.float32),
            in_specs=[pl.BlockSpec(memory_space=pl.ANY)] + [pl.BlockSpec(memory_space=pltpu.VMEM)] * 3,
            out_specs=pl.BlockSpec(memory_space=pltpu.VMEM),
            scratch_shapes=[
                pltpu.VMEM((SLOTS, 2 * piece, 8 * BR), jnp.bfloat16),
                pltpu.VMEM((2, blocks, 4, 2, BR, vecs), jnp.bfloat16),
                pltpu.VMEM((2, chunks, CH, vecs), jnp.bfloat16),
                pltpu.VMEM((2, chunks // 2, CH, vecs), jnp.bfloat16),
                pltpu.VMEM((2, 2 * piece, vecs), jnp.float32),
                pltpu.VMEM((2, piece, vecs), jnp.float32),
                pltpu.VMEM((piece, vecs), jnp.float32),
                pltpu.VMEM((blocks, 128), jnp.float32),
                pltpu.VMEM((piece, 128), jnp.float32),
                pltpu.VMEM((2, 8, vecs), jnp.float32),
                pltpu.VMEM((2, 16, 8, vecs), jnp.float32),
                pltpu.VMEM((8, vecs), jnp.float32),
                sems((SLOTS,)),
            ] + [sems((blocks,))] * 7 + [sems((2,))] + [sems((chunks,))] * 4 + [sems((2, chunks))] * 4
            + [sems((2, chunks // 2))] * 2 + [sems((2, chunks))] * 8
            + [sems((2, 16))] * 2,
            compiler_params=pltpu.CompilerParams(collective_id=0, has_side_effects=True,
                                                 vmem_limit_bytes=67_000_000),
            name='sweeps',
        )(mat_tile, x_piece, tele_piece, dang_rows)

    vec_spec = P(('col', 'row'), None)
    return jax.shard_map(local_sweeps, mesh=mesh,
                         in_specs=(P('row', 'col'), vec_spec, vec_spec, P(('col', 'row'))),
                         out_specs=vec_spec, check_vma=False)
```

```python
import jax
import jax.numpy as jnp
from jax import lax
from jax.experimental import pallas as pl
from jax.experimental.pallas import tpu as pltpu
from jax.sharding import PartitionSpec as P

SWEEPS = 8
DAMPING = 0.85
BR = 128
ENDS = 64
WINDOW = 320
SLOTS = 3
MT = 512
MB = 256
LAG = 2
VAHEAD = 3
MESH = pl.DeviceIdType.MESH


def units_of(piece):
    blocks = piece // BR
    units = []
    for b in range(blocks):
        size = ENDS if b == 0 or b >= blocks - 2 else BR
        units += [(row, size, b, b % 2 == 0 and b < blocks - 5) for row in range(b * BR, (b + 1) * BR, size)]
    return units


def plan(piece):
    units = units_of(piece)
    blocks = piece // BR
    waits, ready, arrived = [], {}, 0.5
    for u, (_, size, b, relay) in enumerate(units):
        n = size / 64
        arrived += 1.75 * n
        waits.append((arrived, 'sum', u))
        back = 0.7 * n + 2.4 + (1.5 if b < blocks - 1 else 0.0)
        if relay:
            now = arrived + 0.7 * n + 2.2
            waits.append((now, 'relay', u))
            now += back
            waits.append((now, 'back_relayed', u))
            now += 0.7 * n + 2.2
            waits.append((now, 'over_relayed', u))
        else:
            now = arrived + back
            waits.append((now, 'back', u))
            now += 1.4 * n + 2.2
            waits.append((now, 'over', u))
        now += 1.4 * n + 2.2
        waits.append((now, 'across', u))
        waits.append((now + 6.0, 'sent', u))
        ready[b] = max(ready.get(b, 0.0), now + 1.5)
    waits += [(ready[b], 'here', b) for b in range(blocks - 1)]
    end = ready[blocks - 1]
    waits = sorted(w for w in waits if w[1] != 'sent' or w[0] < end)
    products = [(b, half) for b in range(blocks - 1) for half in range(2)]
    order, now, landed = [], 0.0, set()
    while waits or products:
        free = bool(products) and products[0][0] in landed
        if free and (not waits or now + 0.5 <= waits[0][0]):
            order.append(('product', products.pop(0)))
            now += 0.85
            continue
        when, what, arg = waits.pop(0)
        order.append((what, arg))
        now = max(now, when) + 0.1
        if what == 'here':
            landed.add(arg)
    return order + [('here', blocks - 1)]


def sweeps_kernel(a_ref, x_ref, v_ref, dang_ref, o_ref,
                  abuf, xbuf, xst, rst, yacc, zr, vperm, dperm, dcol, spart, sbuf, svec,
                  a_sem, g_send, gx_recv, gy_recv, gd_recv, gs_recv, v_send, v_recv, dang_sem, o_send, o_recv, f_send, f_recv,
                  z_send, z_recv, r_send, r_recv, t_send, t_recv, y_send, y_recv, x_send, x_recv,
                  d_send, d_recv, s_send, s_recv):
    i = lax.axis_index('row')
    z = lax.axis_index('col')
    y, x, c = i // 4, (i // 2) % 2, i % 2
    me = z * 8 + i
    home = z == y
    away = z != y
    part = jnp.where(home, 0, 1)
    sib_dev = {'col': z, 'row': i + 1 - 2 * c}
    x_dev = {'col': z, 'row': i + 2 - 4 * x}
    y_row = i + 4 - 8 * y
    y_dev = {'col': z, 'row': y_row}
    z_dev = {'col': 1 - z, 'row': i}
    piece, vecs = o_ref.shape
    blocks = piece // BR
    units = units_of(piece)
    vertices = 16 * piece

    def other(off):
        dev = (me + off) % 16
        return {'col': dev // 8, 'row': dev % 8}, dev

    barrier = pltpu.get_barrier_semaphore()

    @pl.loop(1, 16)
    def _(off):
        dev, _ = other(off)
        pl.semaphore_signal(barrier, inc=1, device_id=dev, device_id_type=MESH)

    def remote(src, dst, send, recv, dev):
        return pltpu.make_async_remote_copy(src_ref=src, dst_ref=dst, send_sem=send, recv_sem=recv,
                                            device_id=dev, device_id_type=MESH)

    def same(ref, send, recv, dev):
        return remote(ref, ref, send, recv, dev)

    def landed(ref, sem):
        pltpu.make_async_copy(ref, ref, sem).wait()

    def at(start, size):
        return pl.ds(pl.multiple_of(start, size), size)

    def rows_of(u):
        return pl.ds(units[u][0], units[u][1])

    def in_block(u):
        return pl.ds(units[u][0] % BR, units[u][1])

    def both(p, u, from_x=x):
        return xbuf.at[p, units[u][2], from_x, c, :, in_block(u)]

    def one(p, u, b):
        return xbuf.at[p, units[u][2], x, c, b, in_block(u)]

    def z_copy(t, u):
        start, size = units[u][:2]
        rows = pl.ds(pl.multiple_of((1 - part) * piece + start, ENDS), size)
        return remote(yacc.at[t, rows], zr.at[t, rows_of(u)], z_send.at[t, u], z_recv.at[t, u], z_dev)

    def z_start(t, first, summed):
        while first < len(units) and units[first][0] + units[first][1] <= units[summed][0] + WINDOW:
            z_copy(t, first).start()
            first += 1
        return first

    def r_copy(p, u):
        return remote(xst.at[p, rows_of(u)], one(p, u, 1), r_send.at[p, u], r_recv.at[p, u], z_dev)

    def to_relay(p, u):
        return remote(xst.at[p, rows_of(u)], rst.at[p, rows_of(u)], r_send.at[p, u], t_recv.at[p, u], y_dev)

    def from_relay(p, u):
        return remote(rst.at[p, rows_of(u)], one(p, u, 1), t_send.at[p, u], r_recv.at[p, u], z_dev)

    def y_copy(p, u, ref):
        return same(ref, y_send.at[p, u], y_recv.at[p, u], y_dev)

    def x_copy(p, u):
        return same(both(p, u), x_send.at[p, u], x_recv.at[p, u], x_dev)

    def d_copy(p, b):
        return same(xbuf.at[p, b, :, c], d_send.at[p, b], d_recv.at[p, b], sib_dev)

    def s_copy(p, off):
        dev, _ = other(off)
        return remote(spart.at[p], sbuf.at[p, me], s_send.at[p, off], s_recv.at[p, me], dev)

    def send_s(p):
        sbuf[p, me] = spart[p]

        @pl.loop(1, 16)
        def _(off):
            s_copy(p, off).start()

    def sum_s(t):
        @pl.loop(1, 16)
        def _(off):
            _, dev = other(off)
            landed(sbuf.at[t, dev], s_recv.at[t, dev])

        s_sum = jnp.sum(sbuf[t].reshape(16 * 8, vecs), axis=0, keepdims=True) / vertices
        svec[...] = jnp.broadcast_to(DAMPING * s_sum + (1.0 - DAMPING), svec.shape)

    def a_start(g):
        q = lax.rem(g, blocks)
        slot = lax.rem(g, SLOTS)
        for b in range(8):
            cols = at(b * piece + q * BR, BR)
            pltpu.make_async_copy(a_ref.at[:, cols], abuf.at[slot, :, pl.ds(b * BR, BR)], a_sem.at[slot]).start()

    def a_next(g):
        @pl.when(g + SLOTS < SWEEPS * blocks)
        def _():
            a_start(g + SLOTS)

    def block_x(p, q):
        return xbuf[p, q].reshape(8 * BR, vecs)

    def multiply(p, b, g, turn):
        slot = lax.rem(g, SLOTS)
        share = piece

        @pl.when(turn == 0)
        def _():
            landed(abuf.at[slot], a_sem.at[slot])

        @pl.loop(0, share // MT)
        def _(m):
            rows = at(turn * share + m * MT, MT)
            yacc[p, rows] += jnp.dot(abuf[slot, rows], block_x(p, b), preferred_element_type=jnp.float32)

        @pl.when(turn == 1)
        def _():
            a_next(g)

    ahead = sum(start + size <= MB for start, size, _, _ in units)

    def multiply_last(p, g):
        slot = lax.rem(g, SLOTS)
        landed(abuf.at[slot], a_sem.at[slot])
        x_last = block_x(p, blocks - 1)

        @pl.loop(0, piece // MB)
        def _(m):
            for which in (1 - part, part):
                rows = at(which * piece + m * MB, MB)
                yacc[p, rows] += jnp.dot(abuf[slot, rows], x_last, preferred_element_type=jnp.float32)

            @pl.when(m == 0)
            def _():
                for u in range(ahead):
                    z_copy(p, u).start()

        a_next(g)

    def clear(p):
        @pl.loop(0, 2 * piece // MB)
        def _(m):
            yacc[p, at(m * MB, MB)] = jnp.zeros((MB, vecs), jnp.float32)

    def new_rows(t, u):
        start, size = units[u][:2]
        mine = pl.ds(pl.multiple_of(part * piece + start, ENDS), size)
        landed(zr.at[t, rows_of(u)], z_recv.at[t, u])
        return DAMPING * (yacc[t, mine] + zr[t, rows_of(u)]) + svec[0:1] * vperm[rows_of(u)]

    def dang_sum(col, rows_f32):
        halves = [col * rows_f32[:, h:h + 128] for h in range(0, vecs, 128)]
        return jnp.sum(jnp.concatenate(halves, axis=1).reshape(-1, 8, vecs), axis=0)

    def dang_col(ref, b):
        return jnp.transpose(jnp.broadcast_to(ref[pl.ds(b, 1)], (BR, 128)))

    @pl.loop(0, SLOTS)
    def _(g):
        a_start(g)

    o_p = 2 * i + part
    o_dev = {'col': o_p // 8, 'row': o_p % 8}
    moves = o_p != me
    stays = o_p == me
    v_row = me // 2
    v_dev = {'col': jnp.where(me % 2 == 0, v_row // 4, 1 - v_row // 4), 'row': v_row}

    def v_copy(b):
        rows = at(b * BR, BR)
        return remote(v_ref.at[rows], vperm.at[rows], v_send.at[b], v_recv.at[b], v_dev)

    dang_copy = remote(dang_ref, dperm, dang_sem.at[0], dang_sem.at[1], v_dev)

    spart[0] = jnp.zeros(spart.shape[1:], jnp.float32)

    @pl.loop(0, blocks)
    def _(b):
        rows_x = x_ref[at(b * BR, BR)]
        xbuf[0, b, y, x, c] = rows_x.astype(jnp.bfloat16)
        spart[0] += dang_sum(dang_col(dang_ref, b), rows_x)

    pl.semaphore_wait(barrier, 15)

    @pl.when(moves)
    def _():
        dang_copy.start()

    @pl.when(stays)
    def _():
        dperm[...] = dang_ref[...]
        vperm[...] = v_ref[...]

    send_s(0)
    clear(0)

    @pl.loop(0, blocks + 3 * LAG)
    def _(step):
        @pl.when(step < blocks)
        def _():
            own = xbuf.at[0, step, y, x, c]
            same(own, g_send.at[step], gx_recv.at[step], x_dev).start()
            same(own, g_send.at[step], gy_recv.at[step], y_dev).start()
            same(own, g_send.at[step], gs_recv.at[step], sib_dev).start()

        @pl.when((step >= LAG) & (step < blocks + LAG))
        def _():
            b = step - LAG
            from_x, from_y = xbuf.at[0, b, y, 1 - x, c], xbuf.at[0, b, 1 - y, x, c]
            landed(from_y, gy_recv.at[b])

            @pl.when(b % 2 == 0)
            def _():
                same(from_y, g_send.at[b], gd_recv.at[b], x_dev).start()

            landed(from_x, gx_recv.at[b])

            @pl.when(b % 2 == 1)
            def _():
                same(from_x, g_send.at[b], gd_recv.at[b], y_dev).start()

            same(from_x, g_send.at[b], gs_recv.at[b], sib_dev).start()
            same(from_y, g_send.at[b], gs_recv.at[b], sib_dev).start()

        @pl.when((step >= 2 * LAG) & (step < blocks + 2 * LAG))
        def _():
            b = step - 2 * LAG
            from_d = xbuf.at[0, b, 1 - y, 1 - x, c]
            landed(from_d, gd_recv.at[b])
            same(from_d, g_send.at[b], gs_recv.at[b], sib_dev).start()

        @pl.when(step >= 3 * LAG)
        def _():
            b = step - 3 * LAG
            landed(xbuf.at[0, b, :, :, 1 - c], gs_recv.at[b])

            @pl.when(b < blocks - 1)
            def _():
                @pl.loop(0, 2)
                def _(turn):
                    multiply(0, b, b, turn)

    @pl.when(moves)
    def _():
        for b in range(VAHEAD):
            v_copy(b).start()

    multiply_last(0, blocks - 1)

    @pl.loop(0, blocks)
    def _(b):
        landed(yacc.at[1, pl.ds(0, 7 * BR // 2)], g_send.at[b])

    @pl.loop(1, 16)
    def _(off):
        s_copy(0, off).wait_send()

    @pl.when(moves)
    def _():
        dang_copy.wait()

    @pl.loop(0, blocks)
    def _(b):
        dcol[at(b * BR, BR)] = dang_col(dperm, b)

    @pl.loop(0, SWEEPS - 1)
    def _(sweep):
        t = lax.rem(sweep, 2)
        p = 1 - t
        sum_s(t)
        spart[p] = jnp.zeros(spart.shape[1:], jnp.float32)

        issued = ahead

        def sent(u):
            z_copy(t, u).wait_send()
            x_copy(p, u).wait_send()

            @pl.when(away)
            def _():
                r_copy(p, u).wait_send()

            if units[u][3]:
                y_copy(p, u, one(p, u, part)).wait_send()

                @pl.when(home)
                def _():
                    from_relay(p, u).wait_send()
            else:
                @pl.when(home)
                def _():
                    y_copy(p, u, both(p, u)).wait_send()

        waiting = list(range(len(units)))
        for what, arg in plan(piece):
            u = arg
            if what == 'sum':
                start, size, b, relay = units[u]
                issued = z_start(t, issued, u)
                if start % BR == 0:
                    @pl.when(moves & (sweep == 0))
                    def _(b=b):
                        if b + VAHEAD < blocks:
                            v_copy(b + VAHEAD).start()
                        v_copy(b).wait_recv()

                rows_new = new_rows(t, u)
                rows_bf = rows_new.astype(jnp.bfloat16)

                @pl.when(home)
                def _():
                    xbuf[p, b, x, c, 0, in_block(u)] = rows_bf

                @pl.when(away)
                def _():
                    xst[p, rows_of(u)] = rows_bf

                spart[p] += dang_sum(dcol[rows_of(u)], rows_new)

                @pl.when(away)
                def _():
                    (to_relay if relay else r_copy)(p, u).start()

                if relay:
                    @pl.when(home)
                    def _():
                        y_copy(p, u, one(p, u, 0)).start()
                if u == len(units) - 1:
                    send_s(p)
                if u == 1:
                    clear(p)
            elif what == 'relay':
                @pl.when(home)
                def _():
                    landed(rst.at[p, rows_of(u)], t_recv.at[p, u])
                    from_relay(p, u).start()
            elif what == 'back':
                @pl.when(home)
                def _():
                    landed(one(p, u, 1), r_recv.at[p, u])
                    y_copy(p, u, both(p, u)).start()
                    x_copy(p, u).start()
            elif what == 'over':
                @pl.when(away)
                def _():
                    landed(both(p, u), y_recv.at[p, u])
                    x_copy(p, u).start()
            elif what == 'back_relayed':
                @pl.when(away)
                def _():
                    landed(one(p, u, 1), r_recv.at[p, u])
                    y_copy(p, u, one(p, u, 1)).start()
                    landed(one(p, u, 0), y_recv.at[p, u])
                    x_copy(p, u).start()
            elif what == 'over_relayed':
                @pl.when(home)
                def _():
                    landed(one(p, u, 1), y_recv.at[p, u])
                    x_copy(p, u).start()
            elif what == 'across':
                landed(both(p, u, 1 - x), x_recv.at[p, u])
                if (units[u][0] + units[u][1]) % BR == 0:
                    d_copy(p, units[u][2]).start()
            elif what == 'here':
                landed(xbuf.at[p, arg, :, 1 - c], d_recv.at[p, arg])
            elif what == 'product':
                multiply(p, arg[0], (sweep + 1) * blocks + arg[0], arg[1])
            else:
                waiting.remove(u)
                sent(u)

        multiply_last(p, (sweep + 1) * blocks + blocks - 1)
        for u in waiting:
            sent(u)

        @pl.loop(0, blocks)
        def _(b):
            d_copy(p, b).wait_send()

        @pl.loop(1, 16)
        def _(off):
            s_copy(p, off).wait_send()

    t = (SWEEPS - 1) % 2

    def o_copy(u):
        rows = rows_of(u)
        return remote(zr.at[t, rows], o_ref.at[rows], o_send.at[u], o_recv.at[u], o_dev)

    def o_to_relay(u):
        rows = rows_of(u)
        return remote(zr.at[t, rows], zr.at[1 - t, rows], o_send.at[u], f_recv.at[u], y_dev)

    def o_from_relay(u):
        rows = rows_of(u)
        dev = 2 * y_row + 1
        return remote(zr.at[1 - t, rows], o_ref.at[rows], f_send.at[u], o_recv.at[u],
                      {'col': dev // 8, 'row': dev % 8})

    sum_s(t)
    issued = ahead
    for what, u in [event for event in plan(piece) if event[0] in ('sum', 'relay')]:
        rows = rows_of(u)
        if what == 'sum':
            issued = z_start(t, issued, u)
            rows_new = new_rows(t, u)

            @pl.when(moves)
            def _():
                zr[t, rows] = rows_new

            if units[u][3]:
                @pl.when(away)
                def _():
                    o_to_relay(u).start()

            @pl.when(moves & (home if units[u][3] else home | away))
            def _():
                o_copy(u).start()

            @pl.when(stays)
            def _():
                o_ref[rows] = rows_new
        else:
            @pl.when(home)
            def _():
                landed(zr.at[1 - t, rows], f_recv.at[u])
                o_from_relay(u).start()

    for u in range(len(units)):
        z_copy(t, u).wait_send()

        @pl.when(moves)
        def _():
            o_copy(u).wait()

        if units[u][3]:
            @pl.when(home)
            def _():
                o_from_relay(u).wait_send()

    @pl.when(moves)
    def _():
        @pl.loop(0, blocks)
        def _(b):
            v_copy(b).wait_send()


def solution(mesh):
    def local_sweeps(mat_tile, x_piece, tele_piece, dang_piece):
        piece, vecs = x_piece.shape
        blocks, exchanges = piece // BR, len(units_of(piece))
        dang_rows = dang_piece.astype(jnp.float32).reshape(blocks, 128)
        sems = pltpu.SemaphoreType.DMA
        return pl.pallas_call(
            sweeps_kernel,
            out_shape=jax.ShapeDtypeStruct((piece, vecs), jnp.float32),
            in_specs=[pl.BlockSpec(memory_space=pl.ANY)] + [pl.BlockSpec(memory_space=pltpu.VMEM)] * 3,
            out_specs=pl.BlockSpec(memory_space=pltpu.VMEM),
            scratch_shapes=[
                pltpu.VMEM((SLOTS, 2 * piece, 8 * BR), jnp.bfloat16),
                pltpu.VMEM((2, blocks, 2, 2, 2, BR, vecs), jnp.bfloat16),
                pltpu.VMEM((2, piece, vecs), jnp.bfloat16),
                pltpu.VMEM((2, piece, vecs), jnp.bfloat16),
                pltpu.VMEM((2, 2 * piece, vecs), jnp.float32),
                pltpu.VMEM((2, piece, vecs), jnp.float32),
                pltpu.VMEM((piece, vecs), jnp.float32),
                pltpu.VMEM((blocks, 128), jnp.float32),
                pltpu.VMEM((piece, 128), jnp.float32),
                pltpu.VMEM((2, 8, vecs), jnp.float32),
                pltpu.VMEM((2, 16, 8, vecs), jnp.float32),
                pltpu.VMEM((8, vecs), jnp.float32),
                sems((SLOTS,)),
            ] + [sems((blocks,))] * 7 + [sems((2,))] + [sems((exchanges,))] * 4 + [sems((2, exchanges))] * 10
            + [sems((2, blocks))] * 2
            + [sems((2, 16))] * 2,
            compiler_params=pltpu.CompilerParams(collective_id=0, has_side_effects=True,
                                                 vmem_limit_bytes=67_000_000),
            name='sweeps',
        )(mat_tile, x_piece, tele_piece, dang_rows)

    vec_spec = P(('col', 'row'), None)
    return jax.shard_map(local_sweeps, mesh=mesh,
                         in_specs=(P('row', 'col'), vec_spec, vec_spec, P(('col', 'row'))),
                         out_specs=vec_spec, check_vma=False)
```

```python
import jax
import jax.numpy as jnp
from jax import lax
from jax.experimental import pallas as pl
from jax.experimental.pallas import tpu as pltpu
from jax.sharding import PartitionSpec as P

SWEEPS = 8
DAMPING = 0.85
CH = 64
BR = 128
AHEAD = 3
TAIL = 2
RELAY, BACK, BACK_RELAYED, OVER_Y, OVER_Y_RELAYED, OVER_X, OVER_X_RELAYED, HERE, HERE_RELAYED = 2, 3, 5, 5, 7, 7, 9, 8, 10
DRAIN = 8
SENT = 11
LAG = 2
FINAL_RELAY = 3
SLOTS = 4
MT = 512
MB = 256
VAHEAD = 3
MESH = pl.DeviceIdType.MESH


def sweeps_kernel(a_ref, x_ref, v_ref, dang_ref, o_ref, pack_ref,
                  abuf, xbuf, xst, rst, yacc, zr, vperm, dperm, dcol, spart, sbuf, svec,
                  a_sem, pack_sem, g_send, gx_recv, gy_recv, gd_recv, gs_recv, v_send, v_recv, dang_sem, o_send, o_recv, f_send, f_recv,
                  z_send, z_recv, r_send, r_recv, t_send, t_recv, y_send, y_recv, x_send, x_recv,
                  d1_send, d1_recv, d2_send, d2_recv, s_send, s_recv):
    i = lax.axis_index('row')
    z = lax.axis_index('col')
    y, x, c = i // 4, (i // 2) % 2, i % 2
    me = z * 8 + i
    home = z == y
    away = z != y
    part = jnp.where(home, 0, 1)
    k_own = 2 * x + c
    k_sib = 2 * x + 1 - c
    k_x = 2 * (1 - x) + c
    k_d = 2 * (1 - x) + 1 - c
    sib_dev = {'col': z, 'row': i + 1 - 2 * c}
    x_dev = {'col': z, 'row': i + 2 - 4 * x}
    y_row = i + 4 - 8 * y
    y_dev = {'col': z, 'row': y_row}
    z_dev = {'col': 1 - z, 'row': i}
    piece, vecs = o_ref.shape
    chunks = piece // CH
    blocks = piece // BR
    per = BR // CH
    vertices = 16 * piece

    def other(off):
        dev = (me + off) % 16
        return {'col': dev // 8, 'row': dev % 8}, dev

    barrier = pltpu.get_barrier_semaphore()

    @pl.loop(1, 16)
    def _(off):
        dev, _ = other(off)
        pl.semaphore_signal(barrier, inc=1, device_id=dev, device_id_type=MESH)

    def remote(src, dst, send, recv, dev):
        return pltpu.make_async_remote_copy(src_ref=src, dst_ref=dst, send_sem=send, recv_sem=recv,
                                            device_id=dev, device_id_type=MESH)

    def same(ref, send, recv, dev):
        return remote(ref, ref, send, recv, dev)

    def landed(ref, sem):
        pltpu.make_async_copy(ref, ref, sem).wait()

    def at(start, size):
        return pl.ds(pl.multiple_of(start, size), size)

    def both(p, q, k):
        return xbuf.at[p, q // per, k, :, at(q % per * CH, CH)]

    def one(p, q, k, b):
        return xbuf.at[p, q // per, k, b, at(q % per * CH, CH)]

    def z_copy(t, q):
        rows = at((1 - part) * piece + q * CH, CH)
        return remote(yacc.at[t, rows], zr.at[t, at(q * CH, CH)], z_send.at[t, q], z_recv.at[t, q], z_dev)

    def relayed(q):
        return (q % 2 == 0) & (q < chunks - TAIL)

    def direct(q):
        return jnp.logical_not(relayed(q))

    def r_copy(p, q):
        return remote(xst.at[p, q], one(p, q, k_own, 1), r_send.at[p, q], r_recv.at[p, q], z_dev)

    def to_relay(p, q):
        return remote(xst.at[p, q], rst.at[p, q // 2], r_send.at[p, q], t_recv.at[p, q // 2], y_dev)

    def from_relay(p, q):
        return remote(rst.at[p, q // 2], one(p, q, k_own, 1), t_send.at[p, q // 2], r_recv.at[p, q], z_dev)

    def y_copy(p, q, ref):
        return same(ref, y_send.at[p, q], y_recv.at[p, q], y_dev)

    def x_copy(p, q, ref):
        return same(ref, x_send.at[p, q], x_recv.at[p, q], x_dev)

    def d1_copy(p, q, ref):
        return same(ref, d1_send.at[p, q], d1_recv.at[p, q], sib_dev)

    def d2_copy(p, q):
        return same(both(p, q, k_x), d2_send.at[p, q], d2_recv.at[p, q], sib_dev)

    def s_copy(p, off):
        dev, _ = other(off)
        return remote(spart.at[p], sbuf.at[p, me], s_send.at[p, off], s_recv.at[p, me], dev)

    def send_s(p):
        sbuf[p, me] = spart[p]

        @pl.loop(1, 16)
        def _(off):
            s_copy(p, off).start()

    def sum_s(t):
        @pl.loop(1, 16)
        def _(off):
            _, dev = other(off)
            landed(sbuf.at[t, dev], s_recv.at[t, dev])

        s_sum = jnp.sum(sbuf[t].reshape(16 * 8, vecs), axis=0, keepdims=True) / vertices
        svec[...] = jnp.broadcast_to(DAMPING * s_sum + (1.0 - DAMPING), svec.shape)

    def a_start(g):
        q = lax.rem(g, blocks)
        slot = lax.rem(g, SLOTS)
        for b in range(8):
            cols = at(b * piece + q * BR, BR)
            pltpu.make_async_copy(a_ref.at[:, cols], abuf.at[slot, :, pl.ds(b * BR, BR)], a_sem.at[slot]).start()

    def a_packed(g):
        slot = lax.rem(g, SLOTS)
        pltpu.make_async_copy(pack_ref.at[lax.rem(g, blocks)], abuf.at[slot], a_sem.at[slot]).start()

    def pack(g):
        slot = lax.rem(g, SLOTS)
        return pltpu.make_async_copy(abuf.at[slot], pack_ref.at[g], pack_sem.at[slot])

    def a_next(g, first):
        if first:
            pack(g).wait()

            @pl.when(g + SLOTS < blocks)
            def _():
                a_start(g + SLOTS)

            @pl.when(g + SLOTS >= blocks)
            def _():
                a_packed(g + SLOTS)
        else:
            @pl.when(g + SLOTS < SWEEPS * blocks)
            def _():
                a_packed(g + SLOTS)

    def block_x(p, q):
        return xbuf[p, q].reshape(8 * BR, vecs)

    def multiply(p, b, g, turn, first=False):
        slot = lax.rem(g, SLOTS)
        share = 2 * piece // per

        @pl.when(turn == 0)
        def _():
            landed(abuf.at[slot], a_sem.at[slot])
            if first:
                pack(g).start()

        @pl.loop(0, share // MT)
        def _(m):
            rows = at(turn * share + m * MT, MT)
            yacc[p, rows] += jnp.dot(abuf[slot, rows], block_x(p, b), preferred_element_type=jnp.float32)

        @pl.when(turn == per - 1)
        def _():
            a_next(g, first)

    def multiply_last(p, g, first=False):
        slot = lax.rem(g, SLOTS)
        landed(abuf.at[slot], a_sem.at[slot])
        if first:
            pack(g).start()
        x_last = block_x(p, blocks - 1)

        @pl.loop(0, piece // MB)
        def _(m):
            for which in (1 - part, part):
                rows = at(which * piece + m * MB, MB)
                yacc[p, rows] += jnp.dot(abuf[slot, rows], x_last, preferred_element_type=jnp.float32)

            @pl.when(m == 0)
            def _():
                for q in range(AHEAD):
                    z_copy(p, q).start()

        a_next(g, first)

    def clear(p):
        @pl.loop(0, 2 * piece // MB)
        def _(m):
            yacc[p, at(m * MB, MB)] = jnp.zeros((MB, vecs), jnp.float32)

    def new_rows(t, q):
        rows = at(q * CH, CH)
        landed(zr.at[t, rows], z_recv.at[t, q])
        return DAMPING * (yacc[t, at(part * piece + q * CH, CH)] + zr[t, rows]) + svec[0:1] * vperm[rows], rows

    def dang_sum(col, rows_f32):
        halves = [col * rows_f32[:, h:h + 128] for h in range(0, vecs, 128)]
        return jnp.sum(jnp.concatenate(halves, axis=1).reshape(-1, 8, vecs), axis=0)

    def dang_col(ref, b):
        return jnp.transpose(jnp.broadcast_to(ref[pl.ds(b, 1)], (BR, 128)))

    @pl.loop(0, SLOTS)
    def _(g):
        a_start(g)

    o_p = 2 * i + part
    o_dev = {'col': o_p // 8, 'row': o_p % 8}
    moves = o_p != me
    stays = o_p == me
    v_row = me // 2
    v_dev = {'col': jnp.where(me % 2 == 0, v_row // 4, 1 - v_row // 4), 'row': v_row}

    def v_copy(b):
        rows = at(b * BR, BR)
        return remote(v_ref.at[rows], vperm.at[rows], v_send.at[b], v_recv.at[b], v_dev)

    dang_copy = remote(dang_ref, dperm, dang_sem.at[0], dang_sem.at[1], v_dev)

    g_own, g_x, g_y, g_d = 2 * y + x, 2 * y + 1 - x, 2 * (1 - y) + x, 2 * (1 - y) + 1 - x
    spart[0] = jnp.zeros(spart.shape[1:], jnp.float32)

    @pl.loop(0, blocks)
    def _(b):
        rows_x = x_ref[at(b * BR, BR)]
        xbuf[0, b, g_own, c] = rows_x.astype(jnp.bfloat16)
        spart[0] += dang_sum(dang_col(dang_ref, b), rows_x)

    pl.semaphore_wait(barrier, 15)

    @pl.when(moves)
    def _():
        dang_copy.start()

    @pl.when(stays)
    def _():
        dperm[...] = dang_ref[...]
        vperm[...] = v_ref[...]

    send_s(0)
    clear(0)

    @pl.loop(0, blocks + 3 * LAG)
    def _(step):
        @pl.when(step < blocks)
        def _():
            own = xbuf.at[0, step, g_own, c]
            same(own, g_send.at[step], gx_recv.at[step], x_dev).start()
            same(own, g_send.at[step], gy_recv.at[step], y_dev).start()
            same(own, g_send.at[step], gs_recv.at[step], sib_dev).start()

        @pl.when((step >= LAG) & (step < blocks + LAG))
        def _():
            b = step - LAG
            from_x, from_y = xbuf.at[0, b, g_x, c], xbuf.at[0, b, g_y, c]
            landed(from_y, gy_recv.at[b])

            @pl.when(b % 2 == 0)
            def _():
                same(from_y, g_send.at[b], gd_recv.at[b], x_dev).start()

            landed(from_x, gx_recv.at[b])

            @pl.when(b % 2 == 1)
            def _():
                same(from_x, g_send.at[b], gd_recv.at[b], y_dev).start()

            same(from_x, g_send.at[b], gs_recv.at[b], sib_dev).start()
            same(from_y, g_send.at[b], gs_recv.at[b], sib_dev).start()

        @pl.when((step >= 2 * LAG) & (step < blocks + 2 * LAG))
        def _():
            b = step - 2 * LAG
            from_d = xbuf.at[0, b, g_d, c]
            landed(from_d, gd_recv.at[b])
            same(from_d, g_send.at[b], gs_recv.at[b], sib_dev).start()

        @pl.when(step >= 3 * LAG)
        def _():
            b = step - 3 * LAG
            landed(xbuf.at[0, b, :, 1 - c], gs_recv.at[b])

            @pl.when(b < blocks - 1)
            def _():
                @pl.loop(0, per)
                def _(turn):
                    multiply(0, b, b, turn, first=True)

    @pl.when(moves)
    def _():
        for b in range(VAHEAD):
            v_copy(b).start()

    multiply_last(0, blocks - 1, first=True)

    @pl.loop(0, blocks)
    def _(b):
        landed(yacc.at[1, pl.ds(0, 7 * BR // 2)], g_send.at[b])

    @pl.loop(1, 16)
    def _(off):
        s_copy(0, off).wait_send()

    @pl.when(moves)
    def _():
        dang_copy.wait()

    @pl.loop(0, blocks)
    def _(b):
        dcol[at(b * BR, BR)] = dang_col(dperm, b)

    @pl.loop(0, SWEEPS - 1)
    def _(sweep):
        t = lax.rem(sweep, 2)
        p = 1 - t
        sum_s(t)
        spart[p] = jnp.zeros(spart.shape[1:], jnp.float32)

        def spread(q, ref):
            y_copy(p, q, ref).start()
            x_copy(p, q, ref).start()
            d1_copy(p, q, ref).start()

        def forward(q, ref):
            landed(ref, y_recv.at[p, q])
            x_copy(p, q, ref).start()
            d1_copy(p, q, ref).start()

        def sent(q):
            z_copy(t, q).wait_send()
            landed(both(p, q, k_own), x_send.at[p, q])
            landed(both(p, q, k_own), d1_send.at[p, q])
            d2_copy(p, q).wait_send()

            @pl.when(away)
            def _():
                r_copy(p, q).wait_send()

            @pl.when(direct(q) & home)
            def _():
                landed(both(p, q, k_own), y_send.at[p, q])

            @pl.when(relayed(q))
            def _():
                landed(one(p, q, k_own, part), y_send.at[p, q])

            @pl.when(relayed(q) & home)
            def _():
                from_relay(p, q).wait_send()

        @pl.loop(0, chunks + DRAIN)
        def _(step):
            def chunk(lag, where):
                q = step - lag
                return q, (q >= 0) & (q < chunks) & where(q)

            @pl.when(step + AHEAD < chunks)
            def _():
                z_copy(t, step + AHEAD).start()

            @pl.when(moves & (sweep == 0) & (step < chunks) & (step % per == 0))
            def _():
                b = step // per

                @pl.when(b + VAHEAD < blocks)
                def _():
                    v_copy(b + VAHEAD).start()

                v_copy(b).wait_recv()

            @pl.when(step < chunks)
            def _():
                q = step
                rows_new, rows = new_rows(t, q)
                rows_bf = rows_new.astype(jnp.bfloat16)

                @pl.when(home)
                def _():
                    xbuf[p, q // per, k_own, 0, at(q % per * CH, CH)] = rows_bf

                @pl.when(away)
                def _():
                    xst[p, q] = rows_bf

                spart[p] += dang_sum(dcol[rows], rows_new)

                @pl.when(away & relayed(q))
                def _():
                    to_relay(p, q).start()

                @pl.when(away & direct(q))
                def _():
                    r_copy(p, q).start()

            @pl.when(step == chunks - 1)
            def _():
                send_s(p)

            q, on = chunk(RELAY, relayed)

            @pl.when(on & home)
            def _():
                landed(rst.at[p, q // 2], t_recv.at[p, q // 2])
                from_relay(p, q).start()
                spread(q, one(p, q, k_own, 0))

            q, on = chunk(BACK, direct)

            @pl.when(on & home)
            def _():
                landed(one(p, q, k_own, 1), r_recv.at[p, q])
                spread(q, both(p, q, k_own))

            q, on = chunk(OVER_Y, direct)

            @pl.when(on & away)
            def _():
                forward(q, both(p, q, k_own))

            q, on = chunk(BACK_RELAYED, relayed)

            @pl.when(on & away)
            def _():
                forward(q, one(p, q, k_own, 0))
                landed(one(p, q, k_own, 1), r_recv.at[p, q])
                spread(q, one(p, q, k_own, 1))

            q, on = chunk(OVER_Y_RELAYED, relayed)

            @pl.when(on & home)
            def _():
                forward(q, one(p, q, k_own, 1))

            for lag, where in ((OVER_X, direct), (OVER_X_RELAYED, relayed)):
                q, on = chunk(lag, where)

                @pl.when(on)
                def _(q=q):
                    landed(both(p, q, k_x), x_recv.at[p, q])
                    d2_copy(p, q).start()

            for lag, where in ((HERE, direct), (HERE_RELAYED, relayed)):
                q, on = chunk(lag, where)

                @pl.when(on)
                def _(q=q):
                    landed(both(p, q, k_sib), d1_recv.at[p, q])
                    landed(both(p, q, k_d), d2_recv.at[p, q])

            @pl.when(step == per)
            def _():
                clear(p)

            turn = step - HERE_RELAYED
            b = turn // per

            @pl.when((turn >= 0) & (b < blocks - 1))
            def _():
                multiply(p, b, (sweep + 1) * blocks + b, turn % per)

            q, on = chunk(SENT, lambda q: True)

            @pl.when(on)
            def _():
                sent(q)

        multiply_last(p, (sweep + 1) * blocks + blocks - 1)

        @pl.loop(chunks + DRAIN - SENT, chunks)
        def _(q):
            sent(q)

        @pl.loop(1, 16)
        def _(off):
            s_copy(p, off).wait_send()

    t = (SWEEPS - 1) % 2

    def o_copy(q):
        rows = at(q * CH, CH)
        return remote(zr.at[t, rows], o_ref.at[rows], o_send.at[q], o_recv.at[q], o_dev)

    def o_to_relay(q):
        rows = at(q * CH, CH)
        return remote(zr.at[t, rows], zr.at[1 - t, rows], o_send.at[q], f_recv.at[q], y_dev)

    def o_from_relay(q):
        rows = at(q * CH, CH)
        dev = 2 * y_row + 1
        return remote(zr.at[1 - t, rows], o_ref.at[rows], f_send.at[q], o_recv.at[q],
                      {'col': dev // 8, 'row': dev % 8})

    sum_s(t)

    @pl.loop(0, chunks + FINAL_RELAY)
    def _(step):
        @pl.when(step + AHEAD < chunks)
        def _():
            z_copy(t, step + AHEAD).start()

        @pl.when(step < chunks)
        def _():
            rows_new, rows = new_rows(t, step)

            @pl.when(moves)
            def _():
                zr[t, rows] = rows_new

            @pl.when(away & relayed(step))
            def _():
                o_to_relay(step).start()

            @pl.when(moves & (home | direct(step)))
            def _():
                o_copy(step).start()

            @pl.when(stays)
            def _():
                o_ref[rows] = rows_new

        q = step - FINAL_RELAY

        @pl.when((q >= 0) & relayed(q) & home)
        def _():
            rows = at(q * CH, CH)
            landed(zr.at[1 - t, rows], f_recv.at[q])
            o_from_relay(q).start()

    @pl.loop(0, chunks)
    def _(q):
        z_copy(t, q).wait_send()

        @pl.when(moves)
        def _():
            o_copy(q).wait()

        @pl.when(relayed(q) & home)
        def _():
            o_from_relay(q).wait_send()

    @pl.when(moves)
    def _():
        @pl.loop(0, blocks)
        def _(b):
            v_copy(b).wait_send()


def solution(mesh):
    def local_sweeps(mat_tile, x_piece, tele_piece, dang_piece):
        piece, vecs = x_piece.shape
        chunks, blocks = piece // CH, piece // BR
        dang_rows = dang_piece.astype(jnp.float32).reshape(blocks, 128)
        sems = pltpu.SemaphoreType.DMA
        out, _ = pl.pallas_call(
            sweeps_kernel,
            out_shape=(jax.ShapeDtypeStruct((piece, vecs), jnp.float32),
                       jax.ShapeDtypeStruct((blocks, 2 * piece, 8 * BR), jnp.bfloat16)),
            in_specs=[pl.BlockSpec(memory_space=pl.ANY)] + [pl.BlockSpec(memory_space=pltpu.VMEM)] * 3,
            out_specs=(pl.BlockSpec(memory_space=pltpu.VMEM), pl.BlockSpec(memory_space=pl.ANY)),
            scratch_shapes=[
                pltpu.VMEM((SLOTS, 2 * piece, 8 * BR), jnp.bfloat16),
                pltpu.VMEM((2, blocks, 4, 2, BR, vecs), jnp.bfloat16),
                pltpu.VMEM((2, chunks, CH, vecs), jnp.bfloat16),
                pltpu.VMEM((2, chunks // 2, CH, vecs), jnp.bfloat16),
                pltpu.VMEM((2, 2 * piece, vecs), jnp.float32),
                pltpu.VMEM((2, piece, vecs), jnp.float32),
                pltpu.VMEM((piece, vecs), jnp.float32),
                pltpu.VMEM((blocks, 128), jnp.float32),
                pltpu.VMEM((piece, 128), jnp.float32),
                pltpu.VMEM((2, 8, vecs), jnp.float32),
                pltpu.VMEM((2, 16, 8, vecs), jnp.float32),
                pltpu.VMEM((8, vecs), jnp.float32),
                sems((SLOTS,)), sems((SLOTS,)),
            ] + [sems((blocks,))] * 7 + [sems((2,))] + [sems((chunks,))] * 4 + [sems((2, chunks))] * 4
            + [sems((2, chunks // 2))] * 2 + [sems((2, chunks))] * 8
            + [sems((2, 16))] * 2,
            compiler_params=pltpu.CompilerParams(collective_id=0, has_side_effects=True,
                                                 vmem_limit_bytes=67_000_000),
            name='sweeps',
        )(mat_tile, x_piece, tele_piece, dang_rows)
        return out

    vec_spec = P(('col', 'row'), None)
    return jax.shard_map(local_sweeps, mesh=mesh,
                         in_specs=(P('row', 'col'), vec_spec, vec_spec, P(('col', 'row'))),
                         out_specs=vec_spec, check_vma=False)
```

```python
import jax
import jax.numpy as jnp
from jax import lax
from jax.experimental import pallas as pl
from jax.experimental.pallas import tpu as pltpu
from jax.sharding import PartitionSpec as P

SWEEPS = 8
DAMPING = 0.85
CH = 64
BR = 128
AHEAD = 4
TAIL = 2
RELAY, BACK, BACK_RELAYED, OVER_Y, OVER_Y_RELAYED, OVER_X, OVER_X_RELAYED, HERE, HERE_RELAYED = 2, 3, 5, 5, 7, 7, 9, 8, 10
DRAIN = 8
SENT = 11
LAG = 2
FINAL_RELAY = 3
SLOTS = 3
MT = 512
MB = 256
VAHEAD = 3
MESH = pl.DeviceIdType.MESH


def sweeps_kernel(a_ref, x_ref, v_ref, dang_ref, o_ref,
                  abuf, xbuf, xst, rst, yacc, zr, vperm, dperm, dcol, spart, sbuf, svec,
                  a_sem, g_send, gx_recv, gy_recv, gd_recv, gs_recv, v_send, v_recv, dang_sem, o_send, o_recv, f_send, f_recv,
                  z_send, z_recv, r_send, r_recv, t_send, t_recv, y_send, y_recv, x_send, x_recv,
                  d1_send, d1_recv, d2_send, d2_recv, s_send, s_recv):
    i = lax.axis_index('row')
    z = lax.axis_index('col')
    y, x, c = i // 4, (i // 2) % 2, i % 2
    me = z * 8 + i
    home = z == y
    away = z != y
    part = jnp.where(home, 0, 1)
    k_own = 2 * x + c
    k_sib = 2 * x + 1 - c
    k_x = 2 * (1 - x) + c
    k_d = 2 * (1 - x) + 1 - c
    sib_dev = {'col': z, 'row': i + 1 - 2 * c}
    x_dev = {'col': z, 'row': i + 2 - 4 * x}
    y_row = i + 4 - 8 * y
    y_dev = {'col': z, 'row': y_row}
    z_dev = {'col': 1 - z, 'row': i}
    piece, vecs = o_ref.shape
    chunks = piece // CH
    blocks = piece // BR
    per = BR // CH
    vertices = 16 * piece

    def other(off):
        dev = (me + off) % 16
        return {'col': dev // 8, 'row': dev % 8}, dev

    barrier = pltpu.get_barrier_semaphore()

    @pl.loop(1, 16)
    def _(off):
        dev, _ = other(off)
        pl.semaphore_signal(barrier, inc=1, device_id=dev, device_id_type=MESH)

    def remote(src, dst, send, recv, dev):
        return pltpu.make_async_remote_copy(src_ref=src, dst_ref=dst, send_sem=send, recv_sem=recv,
                                            device_id=dev, device_id_type=MESH)

    def same(ref, send, recv, dev):
        return remote(ref, ref, send, recv, dev)

    def landed(ref, sem):
        pltpu.make_async_copy(ref, ref, sem).wait()

    def at(start, size):
        return pl.ds(pl.multiple_of(start, size), size)

    def both(p, q, k):
        return xbuf.at[p, q // per, k, :, at(q % per * CH, CH)]

    def one(p, q, k, b):
        return xbuf.at[p, q // per, k, b, at(q % per * CH, CH)]

    def z_copy(t, q):
        rows = at((1 - part) * piece + q * CH, CH)
        return remote(yacc.at[t, rows], zr.at[t, at(q * CH, CH)], z_send.at[t, q], z_recv.at[t, q], z_dev)

    def relayed(q):
        return (q % 2 == 0) & (q < chunks - TAIL)

    def direct(q):
        return jnp.logical_not(relayed(q))

    def r_copy(p, q):
        return remote(xst.at[p, q], one(p, q, k_own, 1), r_send.at[p, q], r_recv.at[p, q], z_dev)

    def to_relay(p, q):
        return remote(xst.at[p, q], rst.at[p, q // 2], r_send.at[p, q], t_recv.at[p, q // 2], y_dev)

    def from_relay(p, q):
        return remote(rst.at[p, q // 2], one(p, q, k_own, 1), t_send.at[p, q // 2], r_recv.at[p, q], z_dev)

    def y_copy(p, q, ref):
        return same(ref, y_send.at[p, q], y_recv.at[p, q], y_dev)

    def x_copy(p, q, ref):
        return same(ref, x_send.at[p, q], x_recv.at[p, q], x_dev)

    def d1_copy(p, q, ref):
        return same(ref, d1_send.at[p, q], d1_recv.at[p, q], sib_dev)

    def d2_copy(p, q):
        return same(both(p, q, k_x), d2_send.at[p, q], d2_recv.at[p, q], sib_dev)

    def s_copy(p, off):
        dev, _ = other(off)
        return remote(spart.at[p], sbuf.at[p, me], s_send.at[p, off], s_recv.at[p, me], dev)

    def send_s(p):
        sbuf[p, me] = spart[p]

        @pl.loop(1, 16)
        def _(off):
            s_copy(p, off).start()

    def sum_s(t):
        @pl.loop(1, 16)
        def _(off):
            _, dev = other(off)
            landed(sbuf.at[t, dev], s_recv.at[t, dev])

        s_sum = jnp.sum(sbuf[t].reshape(16 * 8, vecs), axis=0, keepdims=True) / vertices
        svec[...] = jnp.broadcast_to(DAMPING * s_sum + (1.0 - DAMPING), svec.shape)

    def a_start(g):
        q = lax.rem(g, blocks)
        slot = lax.rem(g, SLOTS)
        for b in range(8):
            cols = at(b * piece + q * BR, BR)
            pltpu.make_async_copy(a_ref.at[:, cols], abuf.at[slot, :, pl.ds(b * BR, BR)], a_sem.at[slot]).start()

    def a_next(g):
        @pl.when(g + SLOTS < SWEEPS * blocks)
        def _():
            a_start(g + SLOTS)

    used = pl.ds(0, 8 * BR)

    def block_x(p, q):
        return xbuf[p, q].reshape(8 * BR, vecs)

    def multiply(p, b, g, turn):
        slot = lax.rem(g, SLOTS)
        share = 2 * piece // per

        @pl.when(turn == 0)
        def _():
            landed(abuf.at[slot, :, used], a_sem.at[slot])

        @pl.loop(0, share // MT)
        def _(m):
            rows = at(turn * share + m * MT, MT)
            yacc[p, rows] += jnp.dot(abuf[slot, rows, used], block_x(p, b), preferred_element_type=jnp.float32)

        @pl.when(turn == per - 1)
        def _():
            a_next(g)

    def multiply_last(p, g):
        slot = lax.rem(g, SLOTS)
        landed(abuf.at[slot, :, used], a_sem.at[slot])
        x_last = block_x(p, blocks - 1)

        @pl.loop(0, piece // MB)
        def _(m):
            for which in (1 - part, part):
                rows = at(which * piece + m * MB, MB)
                yacc[p, rows] += jnp.dot(abuf[slot, rows, used], x_last, preferred_element_type=jnp.float32)

            @pl.when(m == 0)
            def _():
                for q in range(AHEAD):
                    z_copy(p, q).start()

        a_next(g)

    def clear(p):
        @pl.loop(0, 2 * piece // MB)
        def _(m):
            yacc[p, at(m * MB, MB)] = jnp.zeros((MB, vecs), jnp.float32)

    def new_rows(t, q):
        rows = at(q * CH, CH)
        landed(zr.at[t, rows], z_recv.at[t, q])
        return DAMPING * (yacc[t, at(part * piece + q * CH, CH)] + zr[t, rows]) + svec[0:1] * vperm[rows], rows

    def dang_sum(col, rows_f32):
        halves = [col * rows_f32[:, h:h + 128] for h in range(0, vecs, 128)]
        return jnp.sum(jnp.concatenate(halves, axis=1).reshape(-1, 8, vecs), axis=0)

    def dang_col(ref, b):
        return jnp.transpose(jnp.broadcast_to(ref[pl.ds(b, 1)], (BR, 128)))

    @pl.loop(0, SLOTS)
    def _(g):
        a_start(g)

    o_p = 2 * i + part
    o_dev = {'col': o_p // 8, 'row': o_p % 8}
    moves = o_p != me
    stays = o_p == me
    v_row = me // 2
    v_dev = {'col': jnp.where(me % 2 == 0, v_row // 4, 1 - v_row // 4), 'row': v_row}

    def v_copy(b):
        rows = at(b * BR, BR)
        return remote(v_ref.at[rows], vperm.at[rows], v_send.at[b], v_recv.at[b], v_dev)

    dang_copy = remote(dang_ref, dperm, dang_sem.at[0], dang_sem.at[1], v_dev)

    g_own, g_x, g_y, g_d = 2 * y + x, 2 * y + 1 - x, 2 * (1 - y) + x, 2 * (1 - y) + 1 - x
    spart[0] = jnp.zeros(spart.shape[1:], jnp.float32)

    @pl.loop(0, blocks)
    def _(b):
        rows_x = x_ref[at(b * BR, BR)]
        xbuf[0, b, g_own, c] = rows_x.astype(jnp.bfloat16)
        spart[0] += dang_sum(dang_col(dang_ref, b), rows_x)

    pl.semaphore_wait(barrier, 15)

    @pl.when(moves)
    def _():
        dang_copy.start()

    @pl.when(stays)
    def _():
        dperm[...] = dang_ref[...]
        vperm[...] = v_ref[...]

    send_s(0)
    clear(0)

    @pl.loop(0, blocks + 3 * LAG)
    def _(step):
        @pl.when(step < blocks)
        def _():
            own = xbuf.at[0, step, g_own, c]
            same(own, g_send.at[step], gx_recv.at[step], x_dev).start()
            same(own, g_send.at[step], gy_recv.at[step], y_dev).start()
            same(own, g_send.at[step], gs_recv.at[step], sib_dev).start()

        @pl.when((step >= LAG) & (step < blocks + LAG))
        def _():
            b = step - LAG
            from_x, from_y = xbuf.at[0, b, g_x, c], xbuf.at[0, b, g_y, c]
            landed(from_y, gy_recv.at[b])

            @pl.when(b % 2 == 0)
            def _():
                same(from_y, g_send.at[b], gd_recv.at[b], x_dev).start()

            landed(from_x, gx_recv.at[b])

            @pl.when(b % 2 == 1)
            def _():
                same(from_x, g_send.at[b], gd_recv.at[b], y_dev).start()

            same(from_x, g_send.at[b], gs_recv.at[b], sib_dev).start()
            same(from_y, g_send.at[b], gs_recv.at[b], sib_dev).start()

        @pl.when((step >= 2 * LAG) & (step < blocks + 2 * LAG))
        def _():
            b = step - 2 * LAG
            from_d = xbuf.at[0, b, g_d, c]
            landed(from_d, gd_recv.at[b])
            same(from_d, g_send.at[b], gs_recv.at[b], sib_dev).start()

        @pl.when(step >= 3 * LAG)
        def _():
            b = step - 3 * LAG
            landed(xbuf.at[0, b, :, 1 - c], gs_recv.at[b])

            @pl.when(b < blocks - 1)
            def _():
                @pl.loop(0, per)
                def _(turn):
                    multiply(0, b, b, turn)

    @pl.when(moves)
    def _():
        for b in range(VAHEAD):
            v_copy(b).start()

    multiply_last(0, blocks - 1)

    @pl.loop(0, blocks)
    def _(b):
        landed(yacc.at[1, pl.ds(0, 7 * BR // 2)], g_send.at[b])

    @pl.loop(1, 16)
    def _(off):
        s_copy(0, off).wait_send()

    @pl.when(moves)
    def _():
        dang_copy.wait()

    @pl.loop(0, blocks)
    def _(b):
        dcol[at(b * BR, BR)] = dang_col(dperm, b)

    @pl.loop(0, SWEEPS - 1)
    def _(sweep):
        t = lax.rem(sweep, 2)
        p = 1 - t
        sum_s(t)
        spart[p] = jnp.zeros(spart.shape[1:], jnp.float32)

        def spread(q, ref):
            y_copy(p, q, ref).start()
            x_copy(p, q, ref).start()
            d1_copy(p, q, ref).start()

        def forward(q, ref):
            landed(ref, y_recv.at[p, q])
            x_copy(p, q, ref).start()
            d1_copy(p, q, ref).start()

        def sent(q):
            z_copy(t, q).wait_send()
            landed(both(p, q, k_own), x_send.at[p, q])
            landed(both(p, q, k_own), d1_send.at[p, q])
            d2_copy(p, q).wait_send()

            @pl.when(away)
            def _():
                r_copy(p, q).wait_send()

            @pl.when(direct(q) & home)
            def _():
                landed(both(p, q, k_own), y_send.at[p, q])

            @pl.when(relayed(q))
            def _():
                landed(one(p, q, k_own, part), y_send.at[p, q])

            @pl.when(relayed(q) & home)
            def _():
                from_relay(p, q).wait_send()

        @pl.loop(0, chunks + DRAIN)
        def _(step):
            def chunk(lag, where):
                q = step - lag
                return q, (q >= 0) & (q < chunks) & where(q)

            @pl.when(step + AHEAD < chunks)
            def _():
                z_copy(t, step + AHEAD).start()

            @pl.when(moves & (sweep == 0) & (step < chunks) & (step % per == 0))
            def _():
                b = step // per

                @pl.when(b + VAHEAD < blocks)
                def _():
                    v_copy(b + VAHEAD).start()

                v_copy(b).wait_recv()

            @pl.when(step < chunks)
            def _():
                q = step
                rows_new, rows = new_rows(t, q)
                rows_bf = rows_new.astype(jnp.bfloat16)

                @pl.when(home)
                def _():
                    xbuf[p, q // per, k_own, 0, at(q % per * CH, CH)] = rows_bf

                @pl.when(away)
                def _():
                    xst[p, q] = rows_bf

                spart[p] += dang_sum(dcol[rows], rows_new)

                @pl.when(away & relayed(q))
                def _():
                    to_relay(p, q).start()

                @pl.when(away & direct(q))
                def _():
                    r_copy(p, q).start()

            @pl.when(step == chunks - 1)
            def _():
                send_s(p)

            q, on = chunk(RELAY, relayed)

            @pl.when(on & home)
            def _():
                landed(rst.at[p, q // 2], t_recv.at[p, q // 2])
                from_relay(p, q).start()
                spread(q, one(p, q, k_own, 0))

            q, on = chunk(BACK, direct)

            @pl.when(on & home)
            def _():
                landed(one(p, q, k_own, 1), r_recv.at[p, q])
                spread(q, both(p, q, k_own))

            q, on = chunk(OVER_Y, direct)

            @pl.when(on & away)
            def _():
                forward(q, both(p, q, k_own))

            q, on = chunk(BACK_RELAYED, relayed)

            @pl.when(on & away)
            def _():
                forward(q, one(p, q, k_own, 0))
                landed(one(p, q, k_own, 1), r_recv.at[p, q])
                spread(q, one(p, q, k_own, 1))

            q, on = chunk(OVER_Y_RELAYED, relayed)

            @pl.when(on & home)
            def _():
                forward(q, one(p, q, k_own, 1))

            for lag, where in ((OVER_X, direct), (OVER_X_RELAYED, relayed)):
                q, on = chunk(lag, where)

                @pl.when(on)
                def _(q=q):
                    landed(both(p, q, k_x), x_recv.at[p, q])
                    d2_copy(p, q).start()

            for lag, where in ((HERE, direct), (HERE_RELAYED, relayed)):
                q, on = chunk(lag, where)

                @pl.when(on)
                def _(q=q):
                    landed(both(p, q, k_sib), d1_recv.at[p, q])
                    landed(both(p, q, k_d), d2_recv.at[p, q])

            @pl.when(step == per)
            def _():
                clear(p)

            turn = step - HERE_RELAYED
            b = turn // per

            @pl.when((turn >= 0) & (b < blocks - 1))
            def _():
                multiply(p, b, (sweep + 1) * blocks + b, turn % per)

            q, on = chunk(SENT, lambda q: True)

            @pl.when(on)
            def _():
                sent(q)

        multiply_last(p, (sweep + 1) * blocks + blocks - 1)

        @pl.loop(chunks + DRAIN - SENT, chunks)
        def _(q):
            sent(q)

        @pl.loop(1, 16)
        def _(off):
            s_copy(p, off).wait_send()

    t = (SWEEPS - 1) % 2

    def o_copy(q):
        rows = at(q * CH, CH)
        return remote(zr.at[t, rows], o_ref.at[rows], o_send.at[q], o_recv.at[q], o_dev)

    def o_to_relay(q):
        rows = at(q * CH, CH)
        return remote(zr.at[t, rows], zr.at[1 - t, rows], o_send.at[q], f_recv.at[q], y_dev)

    def o_from_relay(q):
        rows = at(q * CH, CH)
        dev = 2 * y_row + 1
        return remote(zr.at[1 - t, rows], o_ref.at[rows], f_send.at[q], o_recv.at[q],
                      {'col': dev // 8, 'row': dev % 8})

    sum_s(t)

    @pl.loop(0, chunks + FINAL_RELAY)
    def _(step):
        @pl.when(step + AHEAD < chunks)
        def _():
            z_copy(t, step + AHEAD).start()

        @pl.when(step < chunks)
        def _():
            rows_new, rows = new_rows(t, step)

            @pl.when(moves)
            def _():
                zr[t, rows] = rows_new

            @pl.when(away & relayed(step))
            def _():
                o_to_relay(step).start()

            @pl.when(moves & (home | direct(step)))
            def _():
                o_copy(step).start()

            @pl.when(stays)
            def _():
                o_ref[rows] = rows_new

        q = step - FINAL_RELAY

        @pl.when((q >= 0) & relayed(q) & home)
        def _():
            rows = at(q * CH, CH)
            landed(zr.at[1 - t, rows], f_recv.at[q])
            o_from_relay(q).start()

    @pl.loop(0, chunks)
    def _(q):
        z_copy(t, q).wait_send()

        @pl.when(moves)
        def _():
            o_copy(q).wait()

        @pl.when(relayed(q) & home)
        def _():
            o_from_relay(q).wait_send()

    @pl.when(moves)
    def _():
        @pl.loop(0, blocks)
        def _(b):
            v_copy(b).wait_send()


def solution(mesh):
    def local_sweeps(mat_tile, x_piece, tele_piece, dang_piece):
        piece, vecs = x_piece.shape
        chunks, blocks = piece // CH, piece // BR
        dang_rows = dang_piece.astype(jnp.float32).reshape(blocks, 128)
        sems = pltpu.SemaphoreType.DMA
        return pl.pallas_call(
            sweeps_kernel,
            out_shape=jax.ShapeDtypeStruct((piece, vecs), jnp.float32),
            in_specs=[pl.BlockSpec(memory_space=pl.ANY)] + [pl.BlockSpec(memory_space=pltpu.VMEM)] * 3,
            out_specs=pl.BlockSpec(memory_space=pltpu.VMEM),
            scratch_shapes=[
                pltpu.VMEM((SLOTS, 2 * piece, 9 * BR), jnp.bfloat16),
                pltpu.VMEM((2, blocks, 4, 2, BR, vecs), jnp.bfloat16),
                pltpu.VMEM((2, chunks, CH, vecs), jnp.bfloat16),
                pltpu.VMEM((2, chunks // 2, CH, vecs), jnp.bfloat16),
                pltpu.VMEM((2, 2 * piece, vecs), jnp.float32),
                pltpu.VMEM((2, piece, vecs), jnp.float32),
                pltpu.VMEM((piece, vecs), jnp.float32),
                pltpu.VMEM((blocks, 128), jnp.float32),
                pltpu.VMEM((piece, 128), jnp.float32),
                pltpu.VMEM((2, 8, vecs), jnp.float32),
                pltpu.VMEM((2, 16, 8, vecs), jnp.float32),
                pltpu.VMEM((8, vecs), jnp.float32),
                sems((SLOTS,)),
            ] + [sems((blocks,))] * 7 + [sems((2,))] + [sems((chunks,))] * 4 + [sems((2, chunks))] * 4
            + [sems((2, chunks // 2))] * 2 + [sems((2, chunks))] * 8
            + [sems((2, 16))] * 2,
            compiler_params=pltpu.CompilerParams(collective_id=0, has_side_effects=True,
                                                 vmem_limit_bytes=67_000_000),
            name='sweeps',
        )(mat_tile, x_piece, tele_piece, dang_rows)

    vec_spec = P(('col', 'row'), None)
    return jax.shard_map(local_sweeps, mesh=mesh,
                         in_specs=(P('row', 'col'), vec_spec, vec_spec, P(('col', 'row'))),
                         out_specs=vec_spec, check_vma=False)
```
